256 devices in a mesh: slot: 8 (over z_hi, x), region: 32 (over z_lo, y, core).
Axes of the slice: x: 4, y: 4, z: 8 (z_hi: 2, z_lo: 4; z = z_hi * 4 + z_lo), core: 2. Of those that a mesh axis runs over, the one named last changes fastest.
Arguments:
- ensemble: bfloat16 [16, 256, 512, 128], P('slot', 'region'), may hold values from -6 to 6
- observations: float32 [16, 256, 1024], P('slot', 'region'), may hold values from -12 to 12
- operator_weight: bfloat16 [1024, 512], replicated, may hold values from -0.25 to 0.25
- obs_precision: float32 [1024], replicated, may hold values from 0.02 to 0.2
- channel_mask: int32 [16, 1024], P('slot'), may hold values 0 or 1
Outputs:
- analysis: bfloat16 [16, 256, 512, 128], P('slot', 'region')
The draws below stay inside these ranges and needn't reach their ends.
All inputs are finite; a program needn't handle non-finite values. No bound on the sum of `channel_mask` on one device may be relied on, other than what follows from the above.
Results may differ from the reference program's by a relative error of at most 0.014.
Values may be sent and summed in bfloat16 or wider, within the bound.
A program may use at most 64 MiB of HBM per device.

```python
import math
import jax
import jax.numpy as jnp
from jax import lax

M = 128
CH = 1024
ROWS = 512
OUTER = 2
NS_STEPS = 8
SLOTS = 16
PATCHES = 256


def draw_ensemble(key, part):
    subspace = max(M // 4, 4)
    subkeys = jax.random.split(jax.random.fold_in(key, 11), 5)
    patterns = jax.random.normal(subkeys[0], (PATCHES, subspace, M), jnp.float32)
    loadings = jax.random.normal(subkeys[1], (SLOTS, PATCHES, ROWS, subspace), jnp.float32)
    noise_part = 0.35 * jax.random.normal(subkeys[3], (SLOTS, PATCHES, ROWS, M), jnp.float32)
    offset = 0.5 * jax.random.normal(subkeys[4], (SLOTS, PATCHES, ROWS, 1), jnp.float32)
    combined = jnp.einsum('tprk,pkm->tprm', loadings, patterns) * (0.9 / math.sqrt(subspace))
    values = combined + noise_part + offset
    return jnp.clip(values, -6.0, 6.0).astype(jnp.bfloat16)


def with_ends(drawn, key, low, high):
    longest = drawn.shape.index(max(drawn.shape))
    spots = []
    for shift in (0, 1):
        where = [jax.random.randint(jax.random.fold_in(key, axis), (), 0, length) for axis, length in enumerate(drawn.shape)]
        where[longest] = (where[longest] + shift) % drawn.shape[longest]
        spots.append(tuple(where))
    return drawn.at[spots[0]].set(low).at[spots[1]].set(high)


def steps_of(stream_key, shape, shards, least, high):
    def one(position, shards_of):
        heights = jax.random.uniform(jax.random.fold_in(jax.random.fold_in(stream_key, 6), position), (shards_of,), jnp.float32, least / len(shards), high / len(shards))
        return jnp.repeat(jnp.exp(heights), shape[position] // shards_of).reshape((-1,) + (1,) * (len(shape) - position - 1))

    loudness = one(*shards[0])
    for cut in shards[1:]:
        loudness = loudness * one(*cut)
    return loudness


def centred(rng, dims, scale, limit, cuts=(), kind=jnp.bfloat16):
    level = steps_of(rng, dims, cuts, -0.22, 0.18) if cuts else 1.0
    result = jax.random.normal(rng, dims, jnp.float32) * scale * level
    return jnp.minimum(jnp.maximum(result, -limit), limit).astype(kind)


def setup_inputs(seed: int = 0) -> dict:
    keys = jax.random.split(jax.random.key(seed), 6)
    ensemble = draw_ensemble(jax.random.fold_in(keys[5], 71), 0)
    observations = centred(keys[1], (SLOTS, PATCHES, CH), 2.0, 12.0, ((0, 8), (1, 32)), jnp.float32)
    operator_weight = centred(keys[2], (CH, ROWS), ROWS ** -0.5, 0.25)
    obs_precision = jnp.clip(jnp.exp(jax.random.uniform(keys[3], (CH,), jnp.float32, math.log(0.02), math.log(0.2))), 0.02, 0.2)
    channel_mask = with_ends((jax.random.randint(keys[4], (SLOTS, CH), 0, 4) < 3).astype(jnp.int32), jax.random.fold_in(keys[4], 1), 0, 1)
    return dict(ensemble=ensemble, observations=observations, operator_weight=operator_weight, obs_precision=obs_precision, channel_mask=channel_mask)


LOCAL_WEIGHT = 0.5

def quad_terms(misfit, weights):
    member_mean = lax.optimization_barrier(jnp.mean(misfit.astype(jnp.float32), axis=-1))
    spread = (misfit.astype(jnp.float32) - member_mean[..., None]).astype(jnp.bfloat16)
    weighted = (weights[:, :, None] * spread.astype(jnp.float32)).astype(jnp.bfloat16)
    innovation = (-weights * member_mean).astype(jnp.bfloat16)
    gram_part = jnp.einsum('tcm,tcn->mn', weighted.astype(jnp.float32), spread.astype(jnp.float32), precision=lax.Precision.HIGHEST)
    grad_part = jnp.einsum('tcm,tc->m', spread.astype(jnp.float32), innovation.astype(jnp.float32), precision=lax.Precision.HIGHEST)
    return jnp.concatenate([gram_part, grad_part[None, :]], axis=0)

def patch_quad(states, observed, operator_weight, weights):
    squashed = jnp.tanh(states.astype(jnp.float32)).astype(jnp.bfloat16)
    predicted = jnp.einsum('cr,trm->tcm', operator_weight.astype(jnp.float32), squashed.astype(jnp.float32), precision=lax.Precision.HIGHEST)
    misfit = (predicted - observed[:, :, None]).astype(jnp.bfloat16)
    return quad_terms(misfit, weights)

def inverse_root(gram):
    members = gram.shape[-1]
    identity = jnp.eye(members, dtype=jnp.float32)
    shifted = gram + (members - 1.0) * identity
    norm_size = jnp.sqrt(lax.optimization_barrier(jnp.sum(shifted * shifted, axis=(1, 2))))
    iterate = shifted / norm_size[:, None, None]
    factor = jnp.broadcast_to(identity, gram.shape)
    for number in range(NS_STEPS):
        middle = 1.5 * identity - 0.5 * jnp.einsum('bij,bjk->bik', factor, iterate, precision=lax.Precision.HIGHEST)
        iterate = jnp.einsum('bij,bjk->bik', iterate, middle, precision=lax.Precision.HIGHEST)
        factor = jnp.einsum('bij,bjk->bik', middle, factor, precision=lax.Precision.HIGHEST)
    return factor / jnp.sqrt(norm_size)[:, None, None]

def transform(totals):
    members = totals.shape[-1]
    gram = totals[:, :members, :]
    grad = totals[:, members, :]
    inv_root = inverse_root(gram)
    inner = jnp.einsum('bij,bj->bi', inv_root, grad, precision=lax.Precision.HIGHEST)
    along = jnp.einsum('bij,bj->bi', inv_root, inner, precision=lax.Precision.HIGHEST)
    return (jnp.sqrt(members - 1.0) * inv_root + along[:, :, None]).astype(jnp.bfloat16)

def apply_mixing(states, mixing):
    centre = lax.optimization_barrier(jnp.mean(states.astype(jnp.float32), axis=-1, keepdims=True))
    deviation = (states.astype(jnp.float32) - centre).astype(jnp.bfloat16)
    moved = jnp.einsum('trm,mn->trn', deviation.astype(jnp.float32), mixing.astype(jnp.float32), precision=lax.Precision.HIGHEST)
    return (centre + moved).astype(jnp.bfloat16)

def reference(ensemble, observations, operator_weight, obs_precision, channel_mask):
    weights = obs_precision[None, :] * channel_mask.astype(jnp.float32) / OUTER
    states = jnp.moveaxis(ensemble, 1, 0)
    observed = jnp.moveaxis(observations, 1, 0)
    for outer_step in range(OUTER):
        quads = lax.map(lambda packed: patch_quad(packed[0], packed[1], operator_weight, weights), (states, observed))
        localized = quads + LOCAL_WEIGHT * (jnp.roll(quads, 1, axis=0) + jnp.roll(quads, -1, axis=0))
        mixing = transform(localized)
        states = lax.map(lambda packed: apply_mixing(packed[0], packed[1]), (states, mixing))
    return jnp.moveaxis(states, 0, 1)
```

```python
import functools
import math

import jax
import jax.numpy as jnp
from jax import lax
from jax.experimental import pallas as pl
from jax.experimental.pallas import tpu as pltpu
from jax.sharding import PartitionSpec as P

OUTER = 2
NS_STEPS = 8
LOCAL_WEIGHT = 0.5
XN = 4

F32 = jnp.float32
BF16 = jnp.bfloat16
MESH = pl.DeviceIdType.MESH
NT = (((1,), (1,)), ((), ()))


def iota(shape, dim):
    return lax.broadcasted_iota(jnp.int32, shape, dim)


def halves(a):
    high = a.astype(BF16)
    return high, (a - high.astype(F32)).astype(BF16)


def product(a, b):
    (ah, al), (bh, bl) = a, b
    return (
        jnp.dot(ah, bl, preferred_element_type=F32)
        + jnp.dot(al, bh, preferred_element_type=F32)
        + jnp.dot(ah, bh, preferred_element_type=F32)
    )


def packed(gram):
    top, bottom = gram[0:64], gram[64:128]
    row, col = iota((64, 128), 0), iota((64, 128), 1)
    body = jnp.where(col >= row, top, pltpu.roll(bottom, 64, 1))
    diag = jnp.sum(jnp.where(col == row + 64, bottom, 0.0), axis=0, keepdims=True)
    tail_row = iota((16, 128), 0)
    grad = gram[128:129] + gram[129:130]
    tail = jnp.where(tail_row == 0, diag, jnp.where(tail_row == 1, grad, 0.0))
    return jnp.concatenate([body, tail], axis=0)


def message(pack):
    tail = pack[64:80]
    row = iota((16, 128), 0)
    grad = tail[1:2] + tail[2:3]
    high = grad.astype(BF16).astype(F32)
    tail = jnp.where(
        row == 0, tail, jnp.where(row == 1, high, jnp.where(row == 2, grad - high, 0.0))
    )
    return jnp.concatenate([pack[0:64].astype(BF16), tail.astype(BF16)], axis=0)


def unpacked(pack):
    top = pack[0:64]
    row, col = iota((64, 128), 0), iota((64, 128), 1)
    upper = jnp.where(col >= row, top, 0.0)
    lower = pltpu.roll(jnp.where(col < row, top, 0.0), 64, 1)
    lower = jnp.where(col == row + 64, pack[64:65], lower)
    half = jnp.concatenate([upper, lower], axis=0)
    row, col = iota((128, 128), 0), iota((128, 128), 1)
    return jnp.where(row == col, half, half + half.T), pack[65:66] + pack[66:67]


def transforms(packs):
    members = 128
    row, col = iota((128, 128), 0), iota((128, 128), 1)
    identity = jnp.where(row == col, 1.0, 0.0).astype(F32)
    grads, scales, iterates, factors = [], [], [], []
    for pack in packs:
        gram, grad = unpacked(pack)
        shifted = gram + (members - 1.0) * identity
        total = jnp.sum(jnp.sum(shifted * shifted, axis=0, keepdims=True), axis=1, keepdims=True)
        norm = jnp.sqrt(total)
        grads.append(grad)
        scales.append(1.0 / jnp.sqrt(norm))
        iterates.append(shifted * (1.0 / norm))
    count = len(packs)
    middles = [1.5 * identity - 0.5 * it for it in iterates]
    split_mid = [halves(m) for m in middles]
    factors = middles
    iterates = [product(halves(iterates[i]), split_mid[i]) for i in range(count)]
    for number in range(1, NS_STEPS):
        split_fac = [halves(f) for f in factors]
        split_it = [halves(it) for it in iterates]
        middles = [
            1.5 * identity - 0.5 * product(split_fac[i], split_it[i]) for i in range(count)
        ]
        split_mid = [halves(m) for m in middles]
        if number + 1 < NS_STEPS:
            iterates = [product(split_it[i], split_mid[i]) for i in range(count)]
        factors = [product(split_mid[i], split_fac[i]) for i in range(count)]
    out = []
    for i in range(count):
        root = factors[i] * scales[i]
        split_root = halves(root)
        grad = jnp.broadcast_to(grads[i], (16, 128))
        inner = product(halves(grad), split_root)
        along = product(halves(inner), split_root)
        out.append((math.sqrt(members - 1.0) * root + along[0:1]).astype(BF16))
    return out


def kernel(
    regions,
    x_hbm, obs_hbm, op_hbm, wt_hbm,
    x1_hbm, mix_out,
    xin, obs, op, wt, opw, amat, bvec,
    sq, sc, dev, cen, zb, pk, x1t, x1v,
    halo_out, halo_in, part, rs_in, z_out, z_in, mixbuf,
    load_sem, store_sem, halo_s, halo_r, rs_s, rs_r, z_s, z_r, ag_s, ag_r,
):
    slot, region = lax.axis_index("slot"), lax.axis_index("region")
    xi, zi = lax.rem(slot, XN), lax.div(slot, XN)
    z_peer = lax.rem(slot + XN, 2 * XN)
    before, after = lax.rem(region + regions - 1, regions), lax.rem(region + 1, regions)

    def x_peer(d):
        return zi * XN + lax.rem(xi + d, XN)

    barrier = pltpu.get_barrier_semaphore()
    for peer in [(x_peer(1), region), (x_peer(2), region), (x_peer(3), region),
                 (z_peer, region), (slot, before), (slot, after)]:
        pl.semaphore_signal(barrier, inc=1, device_id=peer, device_id_type=MESH)

    loads = [
        pltpu.make_async_copy(op_hbm, op, load_sem.at[0]),
        pltpu.make_async_copy(wt_hbm, wt, load_sem.at[1]),
        pltpu.make_async_copy(obs_hbm, obs, load_sem.at[2]),
        pltpu.make_async_copy(x_hbm.at[:, 0:1], xin.at[:, 0:1], load_sem.at[3]),
        pltpu.make_async_copy(x_hbm.at[:, 7:8], xin.at[:, 1:2], load_sem.at[4]),
        pltpu.make_async_copy(x_hbm.at[:, 1:7], xin.at[:, 2:8], load_sem.at[5]),
    ]
    for load in loads:
        load.start()
    for load in loads[:3]:
        load.wait()

    @pl.loop(0, 8)
    def _(ci):
        c = pl.multiple_of(ci * 128, 128)
        weight = [wt[t:t + 1, pl.ds(c, 128)] for t in range(2)]
        for ri in range(4):
            block = op[pl.ds(c, 128), ri * 128:(ri + 1) * 128].astype(F32).T
            for t in range(2):
                opw[t, ri * 128:(ri + 1) * 128, pl.ds(c, 128)] = (block * weight[t]).astype(BF16)

    for t in range(2):
        high, low = halves(obs[t] * wt[t:t + 1, :])
        both = jnp.dot(jnp.concatenate([high, low], axis=0), op[...], preferred_element_type=F32)
        for p in range(8):
            bvec[t, p] = both[p:p + 1] + both[p + 8:p + 9]

    for load in loads[3:]:
        load.wait()

    def squash(block, t, q, column):
        squashed = jnp.tanh(block).astype(BF16)
        wide = squashed.astype(F32)
        mean = jnp.sum(wide, axis=0, keepdims=True) * (1.0 / 128)
        sq[t, pl.ds(pl.multiple_of(q * 128, 128), 128), column * 128:(column + 1) * 128] = squashed
        at = t * 512 + column * 128
        sc[q, :, at:at + 128] = (wide - mean).astype(BF16)

    @pl.loop(0, 4)
    def _(step):
        t, part_row = lax.div(step, 2), pl.multiple_of(lax.rem(step, 2) * 256, 256)
        amat[t, pl.ds(part_row, 256), :] = jnp.dot(
            opw[t, pl.ds(part_row, 256), :], op[...], preferred_element_type=F32
        ).astype(BF16)
        for i in range(2):
            q = 2 * step + i
            for s in range(2):
                for column in range(4):
                    block = xin[s, q, column * 128:(column + 1) * 128, :].astype(F32).T
                    centre = jnp.sum(block, axis=0, keepdims=True) * (1.0 / 128)
                    at = s * 512 + column * 128
                    cen[q, :, at:at + 128] = centre
                    dev[q, :, at:at + 128] = (block - centre).astype(BF16)
                    squash(block, s, q, column)

    def position(p):
        return 0 if p == 0 else 1 if p == 7 else p + 1

    def halo_copies(k):
        return [
            pltpu.make_async_remote_copy(
                src_ref=halo_out.at[k, side], dst_ref=halo_in.at[k, 1 - side],
                send_sem=halo_s.at[k, side], recv_sem=halo_r.at[k, 1 - side],
                device_id=(slot, before if side == 0 else after), device_id_type=MESH,
            )
            for side in range(2)
        ]

    def halo_arrival(k, side):
        return pltpu.make_async_remote_copy(
            src_ref=halo_out.at[k, 1 - side], dst_ref=halo_in.at[k, side],
            send_sem=halo_s.at[k, 1 - side], recv_sem=halo_r.at[k, side],
            device_id=(slot, before if side == 0 else after), device_id_type=MESH,
        )

    def rs_copy(k, j):
        d = lax.rem(j - xi + XN, XN)
        return pltpu.make_async_remote_copy(
            src_ref=part.at[k, j], dst_ref=rs_in.at[k, d - 1],
            send_sem=rs_s.at[k, d - 1], recv_sem=rs_r.at[k, d - 1],
            device_id=(zi * XN + j, region), device_id_type=MESH,
        )

    def localize(k, j):
        for i in range(2):
            p = 2 * j + i
            left = halo_in[k, 0].astype(F32) if p == 0 else pk[position(p - 1)]
            right = halo_in[k, 1].astype(F32) if p == 7 else pk[position(p + 1)]
            part[k, j, i] = message(pk[position(p)] + LOCAL_WEIGHT * (left + right))

        @pl.when(xi != j)
        def _():
            rs_copy(k, j).start()

    def z_copy(k):
        return pltpu.make_async_remote_copy(
            src_ref=z_out.at[k], dst_ref=z_in.at[k], send_sem=z_s.at[k], recv_sem=z_r.at[k],
            device_id=(z_peer, region), device_id_type=MESH,
        )

    def ag_copy(k, d):
        own = pl.ds(2 * xi, 2)
        return pltpu.make_async_remote_copy(
            src_ref=mixbuf.at[k, own], dst_ref=mixbuf.at[k, own],
            send_sem=ag_s.at[k, d - 1], recv_sem=ag_r.at[k, d - 1],
            device_id=(x_peer(d), region), device_id_type=MESH,
        )

    def store(t, q):
        p = 0 if q == 0 else 7 if q == 1 else q - 1
        return pltpu.make_async_copy(x1v.at[t, q], x1_hbm.at[t, p], store_sem.at[t, q])

    for k in range(OUTER):
        @pl.loop(0, 4)
        def _(g):
            p0 = jnp.where(g == 0, 0, 2 * g - 1)
            p1 = jnp.where(g == 0, 7, 2 * g)
            if k > 0:
                for i, p in enumerate((p0, p1)):
                    q = 2 * g + i
                    moved = jnp.dot(mixbuf[k - 1, p], dev[q], preferred_element_type=F32)
                    for t in range(2):
                        for column in range(4):
                            at = t * 512 + column * 128
                            rounded = (cen[q, :, at:at + 128] + moved[:, at:at + 128]).astype(BF16)
                            x1t[q, :, at:at + 128] = rounded
                            squash(rounded.astype(F32), t, q, column)
            for t in range(2):
                lines = pl.ds(pl.multiple_of(g * 256, 256), 256)
                for n in range(2):
                    cols = slice(n * 256, (n + 1) * 256)
                    applied = jnp.dot(sq[t, lines, :], amat[t, :, cols], preferred_element_type=F32)
                    for i, p in enumerate((p0, p1)):
                        z = applied[i * 128:(i + 1) * 128]
                        mean = jnp.sum(z, axis=0, keepdims=True) * (1.0 / 128)
                        at = t * 512 + n * 256
                        zb[i, 0:128, at:at + 256] = (z - mean).astype(BF16)
                        pull = bvec[t, p, :, cols] - mean
                        high = pull.astype(BF16).astype(F32)
                        row = iota((16, 256), 0)
                        tail = jnp.where(row == 0, high, jnp.where(row == 1, pull - high, 0.0))
                        zb[i, 128:144, at:at + 256] = tail.astype(BF16)
            for i in range(2):
                q = 2 * g + i
                gram = lax.dot_general(zb[i], sc[q], NT, preferred_element_type=F32)
                pk[q] = packed(gram)

            @pl.when(g == 0)
            def _():
                for side in range(2):
                    halo_out[k, side] = message(pk[side])
                if k == 0:
                    pl.semaphore_wait(barrier, 6)
                for copy in halo_copies(k):
                    copy.start()

            @pl.when(g == 2)
            def _():
                localize(k, 1)

        localize(k, 2)
        halo_arrival(k, 0).wait_recv()
        localize(k, 0)
        halo_arrival(k, 1).wait_recv()
        localize(k, 3)

        if k == OUTER - 1:
            @pl.loop(0, 8)
            def _(q):
                for t in range(2):
                    for column in range(4):
                        at = t * 512 + column * 128
                        block = x1t[q, :, at:at + 128].astype(F32).T
                        x1v[t, q, column * 128:(column + 1) * 128, :] = block.astype(BF16)
            for t in range(2):
                for q in range(8):
                    store(t, q).start()

        for d in range(1, XN):
            pltpu.make_async_remote_copy(
                src_ref=part.at[k, 0], dst_ref=rs_in.at[k, d - 1],
                send_sem=rs_s.at[k, d - 1], recv_sem=rs_r.at[k, d - 1],
                device_id=(x_peer(d), region), device_id_type=MESH,
            ).wait_recv()
        sums = []
        for i in range(2):
            total = part[k, xi, i].astype(F32)
            for d in range(1, XN):
                total = total + rs_in[k, d - 1, i].astype(F32)
            sums.append(total)
            z_out[k, i] = message(total)
        z_copy(k).start()
        z_copy(k).wait_recv()
        mixes = transforms([sums[i] + z_in[k, i].astype(F32) for i in range(2)])
        for i in range(2):
            mixbuf[k, 2 * xi + i] = mixes[i]
        for d in range(1, XN):
            ag_copy(k, d).start()
        for d in range(1, XN):
            pltpu.make_async_remote_copy(
                src_ref=mixbuf.at[k, pl.ds(2 * xi, 2)],
                dst_ref=mixbuf.at[k, pl.ds(2 * lax.rem(xi + XN - d, XN), 2)],
                send_sem=ag_s.at[k, d - 1], recv_sem=ag_r.at[k, d - 1],
                device_id=(x_peer(d), region), device_id_type=MESH,
            ).wait_recv()

    mix_out[...] = mixbuf[OUTER - 1]
    for k in range(OUTER):
        for copy in halo_copies(k):
            copy.wait_send()
        for d in range(1, XN):
            pltpu.make_async_remote_copy(
                src_ref=part.at[k, 0], dst_ref=rs_in.at[k, d - 1],
                send_sem=rs_s.at[k, d - 1], recv_sem=rs_r.at[k, d - 1],
                device_id=(x_peer(d), region), device_id_type=MESH,
            ).wait_send()
            ag_copy(k, d).wait_send()
        z_copy(k).wait_send()
    for t in range(2):
        for q in range(8):
            store(t, q).wait()


def last_apply(x_ref, mix_ref, out_ref):
    mix = mix_ref[0].astype(F32)
    full = mix + (1.0 - jnp.sum(mix, axis=1, keepdims=True)) * (1.0 / 128)
    high, low = halves(full)
    for t in range(2):
        x = x_ref[t, 0]
        moved = lax.dot_general(x, low, NT, preferred_element_type=F32) + lax.dot_general(
            x, high, NT, preferred_element_type=F32
        )
        out_ref[t, 0] = moved.astype(BF16)


def shards(regions, ensemble, observations, operator_weight, obs_precision, channel_mask):
    weights = obs_precision[None, :] * channel_mask.astype(F32) / OUTER
    slots, patches, rows, members = ensemble.shape
    channels = operator_weight.shape[0]
    anywhere = pl.BlockSpec(memory_space=pl.ANY)
    dma, vmem = pltpu.SemaphoreType.DMA, pltpu.VMEM
    states, mixing = pl.pallas_call(
        functools.partial(kernel, regions),
        out_shape=(
            jax.ShapeDtypeStruct(ensemble.shape, BF16),
            jax.ShapeDtypeStruct((patches, members, members), BF16),
        ),
        in_specs=[anywhere] * 4,
        out_specs=(anywhere, pl.BlockSpec(memory_space=pltpu.VMEM)),
        scratch_shapes=[
            vmem((2, 8, 512, 128), BF16),
            vmem((2, 8, 1024), F32),
            vmem((1024, 512), BF16),
            vmem((2, 1024), F32),
            vmem((2, 512, 1024), BF16),
            vmem((2, 512, 512), BF16),
            vmem((2, 8, 1, 512), F32),
            vmem((2, 1024, 512), BF16),
            vmem((8, 128, 1024), BF16),
            vmem((8, 128, 1024), BF16),
            vmem((8, 1, 1024), F32),
            vmem((2, 144, 1024), BF16),
            vmem((8, 80, 128), F32),
            vmem((8, 128, 1024), BF16),
            vmem((2, 8, 512, 128), BF16),
            vmem((2, 2, 80, 128), BF16),
            vmem((2, 2, 80, 128), BF16),
            vmem((2, XN, 2, 80, 128), BF16),
            vmem((2, XN - 1, 2, 80, 128), BF16),
            vmem((2, 2, 80, 128), BF16),
            vmem((2, 2, 80, 128), BF16),
            vmem((2, 8, 128, 128), BF16),
            dma((6,)), dma((2, 8)),
            dma((2, 2)), dma((2, 2)),
            dma((2, XN - 1)), dma((2, XN - 1)),
            dma((2,)), dma((2,)),
            dma((2, XN - 1)), dma((2, XN - 1)),
        ],
        compiler_params=pltpu.CompilerParams(
            collective_id=0, has_side_effects=True, vmem_limit_bytes=40 << 20
        ),
        name="smoother",
    )(ensemble, observations, operator_weight, weights)
    block = pl.BlockSpec((2, 1, rows, members), lambda p: (0, p, 0, 0))
    return pl.pallas_call(
        last_apply,
        grid=(patches,),
        out_shape=jax.ShapeDtypeStruct(ensemble.shape, BF16),
        in_specs=[block, pl.BlockSpec((1, members, members), lambda p: (p, 0, 0))],
        out_specs=block,
        name="last_apply",
    )(states, mixing)


def solution(mesh):
    return jax.shard_map(
        functools.partial(shards, mesh.shape["region"]),
        mesh=mesh,
        in_specs=(
            P("slot", "region", None, None),
            P("slot", "region", None),
            P(),
            P(),
            P("slot", None),
        ),
        out_specs=P("slot", "region", None, None),
        check_vma=False,
    )
```

```python
import functools
import math

import jax
import jax.numpy as jnp
from jax import lax
from jax.experimental import pallas as pl
from jax.experimental.pallas import tpu as pltpu
from jax.sharding import PartitionSpec as P

OUTER = 2
NS_STEPS = 8
LOCAL_WEIGHT = 0.5
XN = 4

F32 = jnp.float32
BF16 = jnp.bfloat16
MESH = pl.DeviceIdType.MESH
NT = (((1,), (1,)), ((), ()))


def iota(shape, dim):
    return lax.broadcasted_iota(jnp.int32, shape, dim)


def halves(a):
    high = a.astype(BF16)
    return high, (a - high.astype(F32)).astype(BF16)


def product(a, b):
    (ah, al), (bh, bl) = a, b
    return (
        jnp.dot(ah, bl, preferred_element_type=F32)
        + jnp.dot(al, bh, preferred_element_type=F32)
        + jnp.dot(ah, bh, preferred_element_type=F32)
    )


def packed(gram):
    top, bottom = gram[0:64], gram[64:128]
    row, col = iota((64, 128), 0), iota((64, 128), 1)
    body = jnp.where(col >= row, top, pltpu.roll(bottom, 64, 1))
    diag = jnp.sum(jnp.where(col == row + 64, bottom, 0.0), axis=0, keepdims=True)
    tail_row = iota((16, 128), 0)
    grad = gram[128:129] + gram[129:130]
    tail = jnp.where(tail_row == 0, diag, jnp.where(tail_row == 1, grad, 0.0))
    return jnp.concatenate([body, tail], axis=0)


def message(pack):
    tail = pack[64:80]
    row = iota((16, 128), 0)
    grad = tail[1:2] + tail[2:3]
    high = grad.astype(BF16).astype(F32)
    tail = jnp.where(
        row == 0, tail, jnp.where(row == 1, high, jnp.where(row == 2, grad - high, 0.0))
    )
    return jnp.concatenate([pack[0:64].astype(BF16), tail.astype(BF16)], axis=0)


def unpacked(pack):
    top = pack[0:64]
    row, col = iota((64, 128), 0), iota((64, 128), 1)
    upper = jnp.where(col >= row, top, 0.0)
    lower = pltpu.roll(jnp.where(col < row, top, 0.0), 64, 1)
    lower = jnp.where(col == row + 64, pack[64:65], lower)
    half = jnp.concatenate([upper, lower], axis=0)
    row, col = iota((128, 128), 0), iota((128, 128), 1)
    return jnp.where(row == col, half, half + half.T), pack[65:66] + pack[66:67]


def transforms(packs):
    members = 128
    row, col = iota((128, 128), 0), iota((128, 128), 1)
    identity = jnp.where(row == col, 1.0, 0.0).astype(F32)
    grads, scales, iterates, factors = [], [], [], []
    for pack in packs:
        gram, grad = unpacked(pack)
        shifted = gram + (members - 1.0) * identity
        total = jnp.sum(jnp.sum(shifted * shifted, axis=0, keepdims=True), axis=1, keepdims=True)
        norm = jnp.sqrt(total)
        grads.append(grad)
        scales.append(1.0 / jnp.sqrt(norm))
        iterates.append(shifted * (1.0 / norm))
    count = len(packs)
    middles = [1.5 * identity - 0.5 * it for it in iterates]
    split_mid = [halves(m) for m in middles]
    factors = middles
    iterates = [product(halves(iterates[i]), split_mid[i]) for i in range(count)]
    for number in range(1, NS_STEPS):
        split_fac = [halves(f) for f in factors]
        split_it = [halves(it) for it in iterates]
        middles = [
            1.5 * identity - 0.5 * product(split_fac[i], split_it[i]) for i in range(count)
        ]
        split_mid = [halves(m) for m in middles]
        if number + 1 < NS_STEPS:
            iterates = [product(split_it[i], split_mid[i]) for i in range(count)]
        factors = [product(split_mid[i], split_fac[i]) for i in range(count)]
    out = []
    for i in range(count):
        root = factors[i] * scales[i]
        split_root = halves(root)
        grad = jnp.broadcast_to(grads[i], (16, 128))
        inner = product(halves(grad), split_root)
        along = product(halves(inner), split_root)
        out.append((math.sqrt(members - 1.0) * root + along[0:1]).astype(BF16))
    return out


def kernel(
    regions,
    x_hbm, obs_hbm, op_hbm, prec_hbm, mask_hbm,
    x1, mix_out,
    xin, obs, op, prec, mask, wt, opw, amat, bvec,
    sq, sc, dev, cen, zb, pk, x1t,
    halo_out, halo_in, part, rs_in, z_out, z_in, mixbuf,
    load_sem, halo_s, halo_r, rs_s, rs_r, z_s, z_r, ag_s, ag_r,
):
    slot, region = lax.axis_index("slot"), lax.axis_index("region")
    xi, zi = lax.rem(slot, XN), lax.div(slot, XN)
    z_peer = lax.rem(slot + XN, 2 * XN)
    before, after = lax.rem(region + regions - 1, regions), lax.rem(region + 1, regions)

    def x_peer(d):
        return zi * XN + lax.rem(xi + d, XN)

    barrier = pltpu.get_barrier_semaphore()
    for peer in [(x_peer(1), region), (x_peer(2), region), (x_peer(3), region),
                 (z_peer, region), (slot, before), (slot, after)]:
        pl.semaphore_signal(barrier, inc=1, device_id=peer, device_id_type=MESH)

    loads = [
        pltpu.make_async_copy(op_hbm, op, load_sem.at[0]),
        pltpu.make_async_copy(prec_hbm, prec, load_sem.at[1]),
        pltpu.make_async_copy(mask_hbm, mask, load_sem.at[2]),
        pltpu.make_async_copy(obs_hbm, obs, load_sem.at[3]),
        pltpu.make_async_copy(x_hbm.at[:, 0:1], xin.at[:, 0:1], load_sem.at[4]),
        pltpu.make_async_copy(x_hbm.at[:, 7:8], xin.at[:, 1:2], load_sem.at[5]),
        pltpu.make_async_copy(x_hbm.at[:, 1:7], xin.at[:, 2:8], load_sem.at[6]),
    ]
    for load in loads:
        load.start()
    for load in loads[:4]:
        load.wait()
    for ci in range(8):
        cols = slice(ci * 128, (ci + 1) * 128)
        wt[:, cols] = prec[ci:ci + 1, :] * mask[:, cols].astype(F32) * (1.0 / OUTER)

    @pl.loop(0, 8)
    def _(ci):
        c = pl.multiple_of(ci * 128, 128)
        weight = [wt[t:t + 1, pl.ds(c, 128)] for t in range(2)]
        for ri in range(4):
            block = op[pl.ds(c, 128), ri * 128:(ri + 1) * 128].astype(F32).T
            for t in range(2):
                opw[t, ri * 128:(ri + 1) * 128, pl.ds(c, 128)] = (block * weight[t]).astype(BF16)

    for t in range(2):
        high, low = halves(obs[t] * wt[t:t + 1, :])
        both = jnp.dot(jnp.concatenate([high, low], axis=0), op[...], preferred_element_type=F32)
        for p in range(8):
            bvec[t, p] = both[p:p + 1] + both[p + 8:p + 9]

    for load in loads[4:]:
        load.wait()

    def squash(block, t, q, column):
        squashed = jnp.tanh(block).astype(BF16)
        wide = squashed.astype(F32)
        mean = jnp.sum(wide, axis=0, keepdims=True) * (1.0 / 128)
        sq[t, pl.ds(pl.multiple_of(q * 128, 128), 128), column * 128:(column + 1) * 128] = squashed
        at = t * 512 + column * 128
        sc[q, :, at:at + 128] = (wide - mean).astype(BF16)

    @pl.loop(0, 4)
    def _(step):
        t, part_row = lax.div(step, 2), pl.multiple_of(lax.rem(step, 2) * 256, 256)
        amat[t, pl.ds(part_row, 256), :] = jnp.dot(
            opw[t, pl.ds(part_row, 256), :], op[...], preferred_element_type=F32
        ).astype(BF16)
        for i in range(2):
            q = 2 * step + i
            for s in range(2):
                for column in range(4):
                    block = xin[s, q, column * 128:(column + 1) * 128, :].astype(F32).T
                    centre = jnp.sum(block, axis=0, keepdims=True) * (1.0 / 128)
                    at = s * 512 + column * 128
                    cen[q, :, at:at + 128] = centre
                    dev[q, :, at:at + 128] = (block - centre).astype(BF16)
                    squash(block, s, q, column)

    def position(p):
        return 0 if p == 0 else 1 if p == 7 else p + 1

    def halo_copies(k):
        return [
            pltpu.make_async_remote_copy(
                src_ref=halo_out.at[k, side], dst_ref=halo_in.at[k, 1 - side],
                send_sem=halo_s.at[k, side], recv_sem=halo_r.at[k, 1 - side],
                device_id=(slot, before if side == 0 else after), device_id_type=MESH,
            )
            for side in range(2)
        ]

    def halo_arrival(k, side):
        return pltpu.make_async_remote_copy(
            src_ref=halo_out.at[k, 1 - side], dst_ref=halo_in.at[k, side],
            send_sem=halo_s.at[k, 1 - side], recv_sem=halo_r.at[k, side],
            device_id=(slot, before if side == 0 else after), device_id_type=MESH,
        )

    def rs_copy(k, j):
        d = lax.rem(j - xi + XN, XN)
        return pltpu.make_async_remote_copy(
            src_ref=part.at[k, j], dst_ref=rs_in.at[k, d - 1],
            send_sem=rs_s.at[k, d - 1], recv_sem=rs_r.at[k, d - 1],
            device_id=(zi * XN + j, region), device_id_type=MESH,
        )

    def localize(k, j):
        for i in range(2):
            p = 2 * j + i
            left = halo_in[k, 0].astype(F32) if p == 0 else pk[position(p - 1)]
            right = halo_in[k, 1].astype(F32) if p == 7 else pk[position(p + 1)]
            part[k, j, i] = message(pk[position(p)] + LOCAL_WEIGHT * (left + right))

        @pl.when(xi != j)
        def _():
            rs_copy(k, j).start()

    def z_copy(k):
        return pltpu.make_async_remote_copy(
            src_ref=z_out.at[k], dst_ref=z_in.at[k], send_sem=z_s.at[k], recv_sem=z_r.at[k],
            device_id=(z_peer, region), device_id_type=MESH,
        )

    def ag_copy(k, d):
        own = pl.ds(2 * xi, 2)
        return pltpu.make_async_remote_copy(
            src_ref=mixbuf.at[k, own], dst_ref=mixbuf.at[k, own],
            send_sem=ag_s.at[k, d - 1], recv_sem=ag_r.at[k, d - 1],
            device_id=(x_peer(d), region), device_id_type=MESH,
        )

    for k in range(OUTER):
        @pl.loop(0, 4)
        def _(g):
            p0 = jnp.where(g == 0, 0, 2 * g - 1)
            p1 = jnp.where(g == 0, 7, 2 * g)
            if k > 0:
                for i, p in enumerate((p0, p1)):
                    q = 2 * g + i
                    moved = jnp.dot(mixbuf[k - 1, p], dev[q], preferred_element_type=F32)
                    for t in range(2):
                        for column in range(4):
                            at = t * 512 + column * 128
                            rounded = (cen[q, :, at:at + 128] + moved[:, at:at + 128]).astype(BF16)
                            x1t[q, :, at:at + 128] = rounded
                            squash(rounded.astype(F32), t, q, column)
            for t in range(2):
                lines = pl.ds(pl.multiple_of(g * 256, 256), 256)
                for n in range(2):
                    cols = slice(n * 256, (n + 1) * 256)
                    applied = jnp.dot(sq[t, lines, :], amat[t, :, cols], preferred_element_type=F32)
                    for i, p in enumerate((p0, p1)):
                        z = applied[i * 128:(i + 1) * 128]
                        mean = jnp.sum(z, axis=0, keepdims=True) * (1.0 / 128)
                        at = t * 512 + n * 256
                        zb[i, 0:128, at:at + 256] = (z - mean).astype(BF16)
                        pull = bvec[t, p, :, cols] - mean
                        high = pull.astype(BF16).astype(F32)
                        row = iota((16, 256), 0)
                        tail = jnp.where(row == 0, high, jnp.where(row == 1, pull - high, 0.0))
                        zb[i, 128:144, at:at + 256] = tail.astype(BF16)
            for i in range(2):
                q = 2 * g + i
                gram = lax.dot_general(zb[i], sc[q], NT, preferred_element_type=F32)
                pk[q] = packed(gram)

            @pl.when(g == 0)
            def _():
                for side in range(2):
                    halo_out[k, side] = message(pk[side])
                if k == 0:
                    pl.semaphore_wait(barrier, 6)
                for copy in halo_copies(k):
                    copy.start()

            @pl.when(g == 2)
            def _():
                localize(k, 1)

        localize(k, 2)
        halo_arrival(k, 0).wait_recv()
        localize(k, 0)
        halo_arrival(k, 1).wait_recv()
        localize(k, 3)

        if k == OUTER - 1:
            @pl.loop(0, 8)
            def _(q):
                p = jnp.where(q == 0, 0, jnp.where(q == 1, 7, q - 1))
                for t in range(2):
                    for column in range(4):
                        at = t * 512 + column * 128
                        block = x1t[q, :, at:at + 128].astype(F32).T
                        x1[t, p, column * 128:(column + 1) * 128, :] = block.astype(BF16)

        for d in range(1, XN):
            pltpu.make_async_remote_copy(
                src_ref=part.at[k, 0], dst_ref=rs_in.at[k, d - 1],
                send_sem=rs_s.at[k, d - 1], recv_sem=rs_r.at[k, d - 1],
                device_id=(x_peer(d), region), device_id_type=MESH,
            ).wait_recv()
        sums = []
        for i in range(2):
            total = part[k, xi, i].astype(F32)
            for d in range(1, XN):
                total = total + rs_in[k, d - 1, i].astype(F32)
            sums.append(total)
            z_out[k, i] = message(total)
        z_copy(k).start()
        z_copy(k).wait_recv()
        mixes = transforms([sums[i] + z_in[k, i].astype(F32) for i in range(2)])
        for i in range(2):
            mixbuf[k, 2 * xi + i] = mixes[i]
        for d in range(1, XN):
            ag_copy(k, d).start()
        for d in range(1, XN):
            pltpu.make_async_remote_copy(
                src_ref=mixbuf.at[k, pl.ds(2 * xi, 2)],
                dst_ref=mixbuf.at[k, pl.ds(2 * lax.rem(xi + XN - d, XN), 2)],
                send_sem=ag_s.at[k, d - 1], recv_sem=ag_r.at[k, d - 1],
                device_id=(x_peer(d), region), device_id_type=MESH,
            ).wait_recv()

    mix_out[...] = mixbuf[OUTER - 1]
    for k in range(OUTER):
        for copy in halo_copies(k):
            copy.wait_send()
        for d in range(1, XN):
            pltpu.make_async_remote_copy(
                src_ref=part.at[k, 0], dst_ref=rs_in.at[k, d - 1],
                send_sem=rs_s.at[k, d - 1], recv_sem=rs_r.at[k, d - 1],
                device_id=(x_peer(d), region), device_id_type=MESH,
            ).wait_send()
            ag_copy(k, d).wait_send()
        z_copy(k).wait_send()


def last_apply(x_ref, mix_ref, out_hbm, out, sem):
    def copy(p):
        return pltpu.make_async_copy(out.at[:, p], out_hbm.at[:, p], sem.at[p])

    for p in range(out.shape[1]):
        mix = mix_ref[p].astype(F32)
        full = mix + (1.0 - jnp.sum(mix, axis=1, keepdims=True)) * (1.0 / 128)
        both = jnp.concatenate(halves(full), axis=1)
        for t in range(2):
            x = x_ref[t, p]
            twice = jnp.concatenate([x, x], axis=1)
            out[t, p] = lax.dot_general(twice, both, NT, preferred_element_type=F32).astype(BF16)
        copy(p).start()
    for p in range(out.shape[1]):
        copy(p).wait()


def shards(regions, ensemble, observations, operator_weight, obs_precision, channel_mask):
    slots, patches, rows, members = ensemble.shape
    hbm = pl.BlockSpec(memory_space=pltpu.HBM)
    near = pl.BlockSpec(memory_space=pltpu.VMEM)
    dma, vmem = pltpu.SemaphoreType.DMA, pltpu.VMEM
    states, mixing = pl.pallas_call(
        functools.partial(kernel, regions),
        out_shape=(
            jax.ShapeDtypeStruct(ensemble.shape, BF16),
            jax.ShapeDtypeStruct((patches, members, members), BF16),
        ),
        in_specs=[hbm] * 5,
        out_specs=(near, near),
        scratch_shapes=[
            vmem((2, 8, 512, 128), BF16),
            vmem((2, 8, 1024), F32),
            vmem((1024, 512), BF16),
            vmem((8, 128), F32),
            vmem((2, 1024), jnp.int32),
            vmem((2, 1024), F32),
            vmem((2, 512, 1024), BF16),
            vmem((2, 512, 512), BF16),
            vmem((2, 8, 1, 512), F32),
            vmem((2, 1024, 512), BF16),
            vmem((8, 128, 1024), BF16),
            vmem((8, 128, 1024), BF16),
            vmem((8, 1, 1024), F32),
            vmem((2, 144, 1024), BF16),
            vmem((8, 80, 128), F32),
            vmem((8, 128, 1024), BF16),
            vmem((2, 2, 80, 128), BF16),
            vmem((2, 2, 80, 128), BF16),
            vmem((2, XN, 2, 80, 128), BF16),
            vmem((2, XN - 1, 2, 80, 128), BF16),
            vmem((2, 2, 80, 128), BF16),
            vmem((2, 2, 80, 128), BF16),
            vmem((2, 8, 128, 128), BF16),
            dma((7,)),
            dma((2, 2)), dma((2, 2)),
            dma((2, XN - 1)), dma((2, XN - 1)),
            dma((2,)), dma((2,)),
            dma((2, XN - 1)), dma((2, XN - 1)),
        ],
        compiler_params=pltpu.CompilerParams(
            collective_id=0, has_side_effects=True, vmem_limit_bytes=40 << 20
        ),
        name="smoother",
    )(
        *(
            pltpu.with_memory_space_constraint(array, pltpu.HBM)
            for array in (
                ensemble, observations, operator_weight, obs_precision.reshape(8, 128), channel_mask
            )
        )
    )
    return pl.pallas_call(
        last_apply,
        out_shape=jax.ShapeDtypeStruct(ensemble.shape, BF16),
        in_specs=[near, near],
        out_specs=hbm,
        scratch_shapes=[vmem(ensemble.shape, BF16), dma((patches,))],
        compiler_params=pltpu.CompilerParams(vmem_limit_bytes=16 << 20),
        name="last_apply",
    )(states, mixing)


def solution(mesh):
    return jax.shard_map(
        functools.partial(shards, mesh.shape["region"]),
        mesh=mesh,
        in_specs=(
            P("slot", "region", None, None),
            P("slot", "region", None),
            P(),
            P(),
            P("slot", None),
        ),
        out_specs=P("slot", "region", None, None),
        check_vma=False,
    )
```

```python
import functools
import math

import jax
import jax.numpy as jnp
from jax import lax
from jax.experimental import pallas as pl
from jax.experimental.pallas import tpu as pltpu
from jax.sharding import PartitionSpec as P

OUTER = 2
NS_STEPS = 8
LOCAL_WEIGHT = 0.5
XN = 4

F32 = jnp.float32
BF16 = jnp.bfloat16
MESH = pl.DeviceIdType.MESH
NT = (((1,), (1,)), ((), ()))


def iota(shape, dim):
    return lax.broadcasted_iota(jnp.int32, shape, dim)


def halves(a):
    high = a.astype(BF16)
    return high, (a - high.astype(F32)).astype(BF16)


def product(a, b):
    (ah, al), (bh, bl) = a, b
    return (
        jnp.dot(ah, bl, preferred_element_type=F32)
        + jnp.dot(al, bh, preferred_element_type=F32)
        + jnp.dot(ah, bh, preferred_element_type=F32)
    )


def packed(gram):
    top, bottom = gram[0:64], gram[64:128]
    row, col = iota((64, 128), 0), iota((64, 128), 1)
    body = jnp.where(col >= row, top, pltpu.roll(bottom, 64, 1))
    diag = jnp.sum(jnp.where(col == row + 64, bottom, 0.0), axis=0, keepdims=True)
    tail_row = iota((16, 128), 0)
    grad = gram[128:129] + gram[129:130]
    tail = jnp.where(tail_row == 0, diag, jnp.where(tail_row == 1, grad, 0.0))
    return jnp.concatenate([body, tail], axis=0)


def message(pack):
    tail = pack[64:80]
    row = iota((16, 128), 0)
    grad = tail[1:2] + tail[2:3]
    high = grad.astype(BF16).astype(F32)
    tail = jnp.where(
        row == 0, tail, jnp.where(row == 1, high, jnp.where(row == 2, grad - high, 0.0))
    )
    return jnp.concatenate([pack[0:64].astype(BF16), tail.astype(BF16)], axis=0)


def unpacked(pack):
    top = pack[0:64]
    row, col = iota((64, 128), 0), iota((64, 128), 1)
    upper = jnp.where(col >= row, top, 0.0)
    lower = pltpu.roll(jnp.where(col < row, top, 0.0), 64, 1)
    lower = jnp.where(col == row + 64, pack[64:65], lower)
    half = jnp.concatenate([upper, lower], axis=0)
    row, col = iota((128, 128), 0), iota((128, 128), 1)
    return jnp.where(row == col, half, half + half.T), pack[65:66] + pack[66:67]


def transforms(packs):
    members = 128
    row, col = iota((128, 128), 0), iota((128, 128), 1)
    identity = jnp.where(row == col, 1.0, 0.0).astype(F32)
    grads, scales, iterates, factors = [], [], [], []
    for pack in packs:
        gram, grad = unpacked(pack)
        shifted = gram + (members - 1.0) * identity
        total = jnp.sum(jnp.sum(shifted * shifted, axis=0, keepdims=True), axis=1, keepdims=True)
        norm = jnp.sqrt(total)
        grads.append(grad)
        scales.append(1.0 / jnp.sqrt(norm))
        iterates.append(shifted * (1.0 / norm))
    count = len(packs)
    middles = [1.5 * identity - 0.5 * it for it in iterates]
    split_mid = [halves(m) for m in middles]
    factors = middles
    iterates = [product(halves(iterates[i]), split_mid[i]) for i in range(count)]
    for number in range(1, NS_STEPS):
        split_fac = [halves(f) for f in factors]
        split_it = [halves(it) for it in iterates]
        middles = [
            1.5 * identity - 0.5 * product(split_fac[i], split_it[i]) for i in range(count)
        ]
        split_mid = [halves(m) for m in middles]
        if number + 1 < NS_STEPS:
            iterates = [product(split_it[i], split_mid[i]) for i in range(count)]
        factors = [product(split_mid[i], split_fac[i]) for i in range(count)]
    out = []
    for i in range(count):
        root = factors[i] * scales[i]
        split_root = halves(root)
        grad = jnp.broadcast_to(grads[i], (16, 128))
        inner = product(halves(grad), split_root)
        along = product(halves(inner), split_root)
        out.append((math.sqrt(members - 1.0) * root + along[0:1]).astype(BF16))
    return out


def pick(g, values):
    chosen = values[-1]
    for number in range(len(values) - 1):
        chosen = jnp.where(g == number, values[number], chosen)
    return chosen


def kernel(
    regions,
    x_hbm, obs_hbm, op_hbm, prec_hbm, mask_hbm,
    out,
    xin, obs, op, prec, mask, wt, opw, amat, bvec,
    xt, sq, sc, dev, cen, zb, pk, x1,
    halo_out, halo_in, part, rs_in, z_out, z_in, mixbuf,
    load_sem, halo_s, halo_r, rs_s, rs_r, z_s, z_r, ag_s, ag_r,
):
    slot, region = lax.axis_index("slot"), lax.axis_index("region")
    xi, zi = lax.rem(slot, XN), lax.div(slot, XN)
    z_peer = lax.rem(slot + XN, 2 * XN)
    before, after = lax.rem(region + regions - 1, regions), lax.rem(region + 1, regions)

    def at_x(j):
        return zi * XN + j

    def x_peer(d):
        return at_x(lax.rem(xi + d, XN))

    barrier = pltpu.get_barrier_semaphore()

    def greet(device):
        pl.semaphore_signal(barrier, inc=1, device_id=device, device_id_type=MESH)

    for d in range(1, XN):
        greet((x_peer(d), region))
    greet((z_peer, region))
    for edge, neighbour in ((0, before), (XN - 1, after)):
        @pl.when(xi == edge)
        def _():
            for j in range(XN):
                greet((at_x(j), neighbour))

    loads = [
        pltpu.make_async_copy(op_hbm, op, load_sem.at[0]),
        pltpu.make_async_copy(prec_hbm, prec, load_sem.at[1]),
        pltpu.make_async_copy(mask_hbm, mask, load_sem.at[2]),
        pltpu.make_async_copy(obs_hbm, obs, load_sem.at[3]),
        pltpu.make_async_copy(x_hbm, xin, load_sem.at[4]),
    ]
    for load in loads:
        load.start()
    pk[0] = jnp.zeros((80, 128), F32)
    pk[9] = jnp.zeros((80, 128), F32)
    for load in loads[:4]:
        load.wait()
    for ci in range(8):
        cols = slice(ci * 128, (ci + 1) * 128)
        wt[:, cols] = prec[ci:ci + 1, :] * mask[:, cols].astype(F32) * (1.0 / OUTER)

    @pl.loop(0, 8)
    def _(ci):
        c = pl.multiple_of(ci * 128, 128)
        weight = [wt[t:t + 1, pl.ds(c, 128)] for t in range(2)]
        for ri in range(4):
            block = op[pl.ds(c, 128), ri * 128:(ri + 1) * 128].astype(F32).T
            for t in range(2):
                opw[t, ri * 128:(ri + 1) * 128, pl.ds(c, 128)] = (block * weight[t]).astype(BF16)

    for t in range(2):
        high, low = halves(obs[t] * wt[t:t + 1, :])
        both = jnp.dot(jnp.concatenate([high, low], axis=0), op[...], preferred_element_type=F32)
        for p in range(8):
            bvec[t, p] = both[p:p + 1] + both[p + 8:p + 9]

    loads[4].wait()

    def squash(block, t, p, column):
        squashed = jnp.tanh(block).astype(BF16)
        wide = squashed.astype(F32)
        mean = jnp.sum(wide, axis=0, keepdims=True) * (1.0 / 128)
        sq[t, pl.ds(pl.multiple_of(p * 128, 128), 128), column * 128:(column + 1) * 128] = squashed
        at = t * 512 + column * 128
        sc[p, :, at:at + 128] = (wide - mean).astype(BF16)

    @pl.loop(0, 4)
    def _(step):
        t, first = lax.div(step, 2), pl.multiple_of(lax.rem(step, 2) * 256, 256)
        for i in range(2):
            cols = slice(i * 256, (i + 1) * 256)
            amat[t, pl.ds(first, 256), cols] = jnp.dot(
                opw[t, pl.ds(first, 256), :], op[:, cols], preferred_element_type=F32
            ).astype(BF16)
            p = 2 * step + i
            for s in range(2):
                for column in range(4):
                    block = xin[s, p, column * 128:(column + 1) * 128, :].astype(F32).T
                    xt[p, :, s * 512 + column * 128:s * 512 + (column + 1) * 128] = block.astype(BF16)
                    squash(block, s, p, column)

    def halo_copy(k, side):
        return pltpu.make_async_remote_copy(
            src_ref=halo_out.at[k, side], dst_ref=halo_in.at[k, xi],
            send_sem=halo_s.at[k, side], recv_sem=halo_r.at[k, xi],
            device_id=(at_x(XN - 1), before) if side == 0 else (at_x(0), after),
            device_id_type=MESH,
        )

    def halo_arrival(k, j):
        return pltpu.make_async_remote_copy(
            src_ref=halo_out.at[k, 0], dst_ref=halo_in.at[k, j],
            send_sem=halo_s.at[k, 0], recv_sem=halo_r.at[k, j],
            device_id=(at_x(0), after), device_id_type=MESH,
        )

    def rs_copy(k, d):
        return pltpu.make_async_remote_copy(
            src_ref=part.at[k, d - 1], dst_ref=rs_in.at[k, d - 1],
            send_sem=rs_s.at[k, d - 1], recv_sem=rs_r.at[k, d - 1],
            device_id=(x_peer(d), region), device_id_type=MESH,
        )

    def localized(p):
        return pk[p + 1] + LOCAL_WEIGHT * (pk[p] + pk[p + 2])

    def send_share(k, d):
        j = lax.rem(xi + d, XN)
        for i in range(2):
            part[k, d - 1, i] = message(localized(2 * j + i))
        rs_copy(k, d).start()

    def z_copy(k):
        return pltpu.make_async_remote_copy(
            src_ref=z_out.at[k], dst_ref=z_in.at[k], send_sem=z_s.at[k], recv_sem=z_r.at[k],
            device_id=(z_peer, region), device_id_type=MESH,
        )

    def ag_copy(k, d):
        own = pl.ds(2 * xi, 2)
        return pltpu.make_async_remote_copy(
            src_ref=mixbuf.at[k, own], dst_ref=mixbuf.at[k, own],
            send_sem=ag_s.at[k, d - 1], recv_sem=ag_r.at[k, d - 1],
            device_id=(x_peer(d), region), device_id_type=MESH,
        )

    def await_pair(k, g):
        ahead = pick(g, (0, 1, 3, 2))

        @pl.when(g > 0)
        def _():
            d = XN - ahead
            other = pl.ds(2 * lax.rem(xi + ahead, XN), 2)
            pltpu.make_async_remote_copy(
                src_ref=mixbuf.at[k, other], dst_ref=mixbuf.at[k, other],
                send_sem=ag_s.at[k, d - 1], recv_sem=ag_r.at[k, d - 1],
                device_id=(x_peer(1), region), device_id_type=MESH,
            ).wait_recv()

        return lax.rem(xi + ahead, XN)

    for k in range(OUTER):
        @pl.loop(0, 4)
        def _(g):
            if k > 0:
                j = await_pair(k - 1, g)
                for i in range(2):
                    p = 2 * j + i
                    moved = jnp.dot(mixbuf[k - 1, p], dev[p], preferred_element_type=F32)
                    for t in range(2):
                        for column in range(4):
                            at = t * 512 + column * 128
                            rounded = (cen[p, :, at:at + 128] + moved[:, at:at + 128]).astype(BF16)
                            xt[p, :, at:at + 128] = rounded
                            squash(rounded.astype(F32), t, p, column)
            else:
                j = pick(g, (0, 3, 1, 2))
            for t in range(2):
                lines = pl.ds(pl.multiple_of(j * 256, 256), 256)
                for n in range(2):
                    cols = slice(n * 256, (n + 1) * 256)
                    applied = jnp.dot(sq[t, lines, :], amat[t, :, cols], preferred_element_type=F32)
                    for i in range(2):
                        z = applied[i * 128:(i + 1) * 128]
                        mean = jnp.sum(z, axis=0, keepdims=True) * (1.0 / 128)
                        at = t * 512 + n * 256
                        zb[i, 0:128, at:at + 256] = (z - mean).astype(BF16)
                        pull = bvec[t, 2 * j + i, :, cols] - mean
                        high = pull.astype(BF16).astype(F32)
                        row = iota((16, 256), 0)
                        tail = jnp.where(row == 0, high, jnp.where(row == 1, pull - high, 0.0))
                        zb[i, 128:144, at:at + 256] = tail.astype(BF16)
            for i in range(2):
                p = 2 * j + i
                gram = lax.dot_general(zb[i], sc[p], NT, preferred_element_type=F32)
                pk[p + 1] = packed(gram)

            if k == 0:
                @pl.when(g == 0)
                def _():
                    pl.semaphore_wait(barrier, XN + 2)

            for side, edge in ((0, 0), (1, XN - 1)):
                @pl.when(j == edge)
                def _():
                    halo_out[k, side] = message(pk[1 + 7 * side])
                    halo_copy(k, side).start()

        for d in (2, 1, 3):
            send_share(k, d)

        if k == 0:
            @pl.loop(0, 8)
            def _(p):
                for column in range(8):
                    cols = slice(column * 128, (column + 1) * 128)
                    block = xt[p, :, cols].astype(F32)
                    centre = jnp.sum(block, axis=0, keepdims=True) * (1.0 / 128)
                    cen[p, :, cols] = centre
                    dev[p, :, cols] = (block - centre).astype(BF16)
        else:
            @pl.loop(0, 8)
            def _(p):
                for t in range(2):
                    for column in range(4):
                        at = t * 512 + column * 128
                        block = xt[p, :, at:at + 128].astype(F32).T
                        x1[t, p, column * 128:(column + 1) * 128, :] = block.astype(BF16)

        sums = [localized(2 * xi + i) for i in range(2)]
        for d in (1, 3, 2):
            rs_copy(k, d).wait_recv()
            for i in range(2):
                sums[i] = sums[i] + rs_in[k, d - 1, i].astype(F32)
        for i in range(2):
            pk[10 + i] = sums[i]
        for edge, i in ((0, 0), (XN - 1, 1)):
            @pl.when(xi == edge)
            def _():
                total = pk[10 + i]
                for j in range(XN):
                    halo_arrival(k, j).wait_recv()
                    total = total + LOCAL_WEIGHT * halo_in[k, j].astype(F32)
                pk[10 + i] = total
        for i in range(2):
            z_out[k, i] = message(pk[10 + i])
        z_copy(k).start()
        z_copy(k).wait_recv()
        mixes = transforms([pk[10 + i] + z_in[k, i].astype(F32) for i in range(2)])
        for i in range(2):
            mixbuf[k, 2 * xi + i] = mixes[i]
        for d in (2, 1, 3):
            ag_copy(k, d).start()

    @pl.loop(0, 4)
    def _(g):
        j = await_pair(OUTER - 1, g)
        for i in range(2):
            p = 2 * j + i
            mix = mixbuf[OUTER - 1, p].astype(F32)
            full = mix + (1.0 - jnp.sum(mix, axis=1, keepdims=True)) * (1.0 / 128)
            both = jnp.concatenate(halves(full), axis=1)
            for t in range(2):
                x = x1[t, p]
                twice = jnp.concatenate([x, x], axis=1)
                moved = lax.dot_general(twice, both, NT, preferred_element_type=F32)
                out[t, p] = moved.astype(BF16)

    for k in range(OUTER):
        for side in range(2):
            halo_copy(k, side).wait_send()
        for d in range(1, XN):
            rs_copy(k, d).wait_send()
            ag_copy(k, d).wait_send()
        z_copy(k).wait_send()


def shards(regions, ensemble, observations, operator_weight, obs_precision, channel_mask):
    slots, patches, rows, members = ensemble.shape
    hbm = pl.BlockSpec(memory_space=pltpu.HBM)
    near = pl.BlockSpec(memory_space=pltpu.VMEM)
    dma, vmem = pltpu.SemaphoreType.DMA, pltpu.VMEM
    return pl.pallas_call(
        functools.partial(kernel, regions),
        out_shape=jax.ShapeDtypeStruct(ensemble.shape, BF16),
        in_specs=[hbm] * 5,
        out_specs=near,
        scratch_shapes=[
            vmem((2, 8, 512, 128), BF16),
            vmem((2, 8, 1024), F32),
            vmem((1024, 512), BF16),
            vmem((8, 128), F32),
            vmem((2, 1024), jnp.int32),
            vmem((2, 1024), F32),
            vmem((2, 512, 1024), BF16),
            vmem((2, 512, 512), BF16),
            vmem((2, 8, 1, 512), F32),
            vmem((8, 128, 1024), BF16),
            vmem((2, 1024, 512), BF16),
            vmem((8, 128, 1024), BF16),
            vmem((8, 128, 1024), BF16),
            vmem((8, 1, 1024), F32),
            vmem((2, 144, 1024), BF16),
            vmem((12, 80, 128), F32),
            vmem((2, 8, 512, 128), BF16),
            vmem((2, 2, 80, 128), BF16),
            vmem((2, XN, 80, 128), BF16),
            vmem((2, XN - 1, 2, 80, 128), BF16),
            vmem((2, XN - 1, 2, 80, 128), BF16),
            vmem((2, 2, 80, 128), BF16),
            vmem((2, 2, 80, 128), BF16),
            vmem((2, 8, 128, 128), BF16),
            dma((5,)),
            dma((2, 2)), dma((2, XN)),
            dma((2, XN - 1)), dma((2, XN - 1)),
            dma((2,)), dma((2,)),
            dma((2, XN - 1)), dma((2, XN - 1)),
        ],
        compiler_params=pltpu.CompilerParams(
            collective_id=0, has_side_effects=True, vmem_limit_bytes=40 << 20
        ),
        name="smoother",
    )(
        *(
            pltpu.with_memory_space_constraint(array, pltpu.HBM)
            for array in (
                ensemble, observations, operator_weight, obs_precision.reshape(8, 128), channel_mask
            )
        )
    )


def solution(mesh):
    return jax.shard_map(
        functools.partial(shards, mesh.shape["region"]),
        mesh=mesh,
        in_specs=(
            P("slot", "region", None, None),
            P("slot", "region", None),
            P(),
            P(),
            P("slot", None),
        ),
        out_specs=P("slot", "region", None, None),
        check_vma=False,
    )
```

```python
import functools
import math

import jax
import jax.numpy as jnp
from jax import lax
from jax.experimental import pallas as pl
from jax.experimental.pallas import tpu as pltpu
from jax.sharding import PartitionSpec as P

OUTER = 2
NS_STEPS = 8
LOCAL_WEIGHT = 0.5
XN = 4

F32 = jnp.float32
BF16 = jnp.bfloat16
MESH = pl.DeviceIdType.MESH
NT = (((1,), (1,)), ((), ()))


def iota(shape, dim):
    return lax.broadcasted_iota(jnp.int32, shape, dim)


def halves(a):
    high = a.astype(BF16)
    return high, (a - high.astype(F32)).astype(BF16)


def product(a, b):
    (ah, al), (bh, bl) = a, b
    left = jnp.concatenate([ah, al], axis=1)
    right = jnp.concatenate(
        [jnp.concatenate([bh, bl], axis=1), jnp.concatenate([bh, jnp.zeros_like(bl)], axis=1)],
        axis=0,
    )
    both = jnp.dot(left, right, preferred_element_type=F32)
    return both[:, 0:128] + both[:, 128:256]


def first_term(a, b):
    return jnp.dot(a[0], b[0], preferred_element_type=F32)


def packed(raw):
    first = jnp.sum(raw[0:128], axis=0, keepdims=True) * (1.0 / 128)
    pull = jnp.broadcast_to(raw[128:129] + raw[129:130], (8, 128))
    gram = jnp.concatenate([raw[0:128], pull], axis=0) - first
    gram = gram - jnp.sum(gram, axis=1, keepdims=True) * (1.0 / 128)
    top, bottom = gram[0:64], gram[64:128]
    row, col = iota((64, 128), 0), iota((64, 128), 1)
    body = jnp.where(col >= row, top, pltpu.roll(bottom, 64, 1))
    diag = jnp.sum(jnp.where(col == row + 64, bottom, 0.0), axis=0, keepdims=True)
    tail_row = iota((16, 128), 0)
    grad = gram[128:129]
    tail = jnp.where(tail_row == 0, diag, jnp.where(tail_row == 1, grad, 0.0))
    return jnp.concatenate([body, tail], axis=0)


def message(pack):
    tail = pack[64:80]
    row = iota((16, 128), 0)
    grad = tail[1:2] + tail[2:3]
    high = grad.astype(BF16).astype(F32)
    tail = jnp.where(
        row == 0, tail, jnp.where(row == 1, high, jnp.where(row == 2, grad - high, 0.0))
    )
    return jnp.concatenate([pack[0:64].astype(BF16), tail.astype(BF16)], axis=0)


def unpacked(pack):
    top = pack[0:64]
    row, col = iota((64, 128), 0), iota((64, 128), 1)
    upper = jnp.where(col >= row, top, 0.0)
    lower = pltpu.roll(jnp.where(col < row, top, 0.0), 64, 1)
    lower = jnp.where(col == row + 64, pack[64:65], lower)
    half = jnp.concatenate([upper, lower], axis=0)
    row, col = iota((128, 128), 0), iota((128, 128), 1)
    return jnp.where(row == col, half, half + half.T), pack[65:66] + pack[66:67]


def transforms(packs):
    members = 128
    row, col = iota((128, 128), 0), iota((128, 128), 1)
    identity = jnp.where(row == col, 1.0, 0.0).astype(F32)
    grads, scales, iterates, factors = [], [], [], []
    for pack in packs:
        gram, grad = unpacked(pack)
        shifted = gram + (members - 1.0) * identity
        total = jnp.sum(jnp.sum(shifted * shifted, axis=0, keepdims=True), axis=1, keepdims=True)
        norm = jnp.sqrt(total)
        grads.append(grad)
        scales.append(1.0 / jnp.sqrt(norm))
        iterates.append(shifted * (1.0 / norm))
    count = len(packs)
    middles = [1.5 * identity - 0.5 * it for it in iterates]
    split_mid = [halves(m) for m in middles]
    factors = middles
    iterates = [product(halves(iterates[i]), split_mid[i]) for i in range(count)]
    for number in range(1, NS_STEPS):
        split_fac = [halves(f) for f in factors]
        split_it = [halves(it) for it in iterates]
        multiply = first_term if number < NS_STEPS - 2 else product
        middles = [
            1.5 * identity - 0.5 * multiply(split_fac[i], split_it[i]) for i in range(count)
        ]
        split_mid = [halves(m) for m in middles]
        if number + 1 < NS_STEPS:
            iterates = [product(split_it[i], split_mid[i]) for i in range(count)]
        factors = [product(split_mid[i], split_fac[i]) for i in range(count)]
    out = []
    for i in range(count):
        root = factors[i] * scales[i]
        split_root = halves(root)
        grad = jnp.broadcast_to(grads[i], (16, 128))
        inner = product(halves(grad), split_root)
        along = product(halves(inner), split_root)
        out.append((math.sqrt(members - 1.0) * root + along[0:1]).astype(BF16))
    return out


def pick(g, values):
    chosen = values[-1]
    for number in range(len(values) - 1):
        chosen = jnp.where(g == number, values[number], chosen)
    return chosen


def kernel(
    regions,
    x_hbm, obs_hbm, op_hbm, prec_hbm, mask_hbm,
    out,
    xin, obs, op, prec, mask, wt, opw, amat,
    sr, sq, dev, cen, zb, pk, x1,
    halo_out, halo_in, part, rs_in, z_out, z_in, mixbuf,
    load_sem, halo_s, halo_r, rs_s, rs_r, z_s, z_r, ag_s, ag_r,
):
    slot, region = lax.axis_index("slot"), lax.axis_index("region")
    xi, zi = lax.rem(slot, XN), lax.div(slot, XN)
    z_peer = lax.rem(slot + XN, 2 * XN)
    before, after = lax.rem(region + regions - 1, regions), lax.rem(region + 1, regions)

    def at_x(j):
        return zi * XN + j

    def x_peer(d):
        return at_x(lax.rem(xi + d, XN))

    barrier = pltpu.get_barrier_semaphore()

    def greet(device):
        pl.semaphore_signal(barrier, inc=1, device_id=device, device_id_type=MESH)

    for d in range(1, XN):
        greet((x_peer(d), region))
    greet((z_peer, region))
    for edge, neighbour in ((0, before), (XN - 1, after)):
        @pl.when(xi == edge)
        def _():
            for j in range(XN):
                greet((at_x(j), neighbour))

    loads = [
        pltpu.make_async_copy(op_hbm, op, load_sem.at[0]),
        pltpu.make_async_copy(prec_hbm, prec, load_sem.at[1]),
        pltpu.make_async_copy(mask_hbm, mask, load_sem.at[2]),
        pltpu.make_async_copy(obs_hbm, obs, load_sem.at[3]),
        pltpu.make_async_copy(x_hbm, xin, load_sem.at[4]),
    ]
    for load in loads:
        load.start()
    pk[0] = jnp.zeros((80, 128), F32)
    pk[9] = jnp.zeros((80, 128), F32)
    for load in loads[:4]:
        load.wait()
    for ci in range(8):
        cols = slice(ci * 128, (ci + 1) * 128)
        wt[:, cols] = prec[ci:ci + 1, :] * mask[:, cols].astype(F32) * (1.0 / OUTER)

    @pl.loop(0, 8)
    def _(ci):
        c = pl.multiple_of(ci * 128, 128)
        weight = [wt[t:t + 1, pl.ds(c, 128)] for t in range(2)]
        for ri in range(4):
            block = op[pl.ds(c, 128), ri * 128:(ri + 1) * 128].astype(F32).T
            for t in range(2):
                opw[t, ri * 128:(ri + 1) * 128, pl.ds(c, 128)] = (block * weight[t]).astype(BF16)

    for t in range(2):
        high, low = halves(obs[t] * wt[t:t + 1, :])
        both = jnp.dot(jnp.concatenate([high, low], axis=0), op[...], preferred_element_type=F32)
        row = iota((16, 512), 0)
        for p in range(8):
            pull = both[p:p + 1] + both[p + 8:p + 9]
            high = pull.astype(BF16).astype(F32)
            tail = jnp.where(row == 0, high, jnp.where(row == 1, pull - high, 0.0))
            zb[p, 128:144, t * 512:(t + 1) * 512] = tail.astype(BF16)

    loads[4].wait()

    @pl.loop(0, 4)
    def _(step):
        t, first = lax.div(step, 2), pl.multiple_of(lax.rem(step, 2) * 256, 256)
        for i in range(2):
            cols = slice(i * 256, (i + 1) * 256)
            amat[t, pl.ds(first, 256), cols] = jnp.dot(
                opw[t, pl.ds(first, 256), :], op[:, cols], preferred_element_type=F32
            ).astype(BF16)
            p = 2 * step + i
            for s in range(2):
                for column in range(4):
                    rows = slice(column * 128, (column + 1) * 128)
                    squashed = jnp.tanh(xin[s, p, rows, :].astype(F32))
                    sr[s, p, rows, :] = squashed.astype(BF16)
                    sq[s, pl.ds(pl.multiple_of(p * 128, 128), 128), rows] = squashed.T.astype(BF16)

    def halo_copy(k, side):
        return pltpu.make_async_remote_copy(
            src_ref=halo_out.at[k, side], dst_ref=halo_in.at[k, xi],
            send_sem=halo_s.at[k, side], recv_sem=halo_r.at[k, xi],
            device_id=(at_x(XN - 1), before) if side == 0 else (at_x(0), after),
            device_id_type=MESH,
        )

    def halo_arrival(k, j):
        return pltpu.make_async_remote_copy(
            src_ref=halo_out.at[k, 0], dst_ref=halo_in.at[k, j],
            send_sem=halo_s.at[k, 0], recv_sem=halo_r.at[k, j],
            device_id=(at_x(0), after), device_id_type=MESH,
        )

    def rs_copy(k, d):
        return pltpu.make_async_remote_copy(
            src_ref=part.at[k, d - 1], dst_ref=rs_in.at[k, d - 1],
            send_sem=rs_s.at[k, d - 1], recv_sem=rs_r.at[k, d - 1],
            device_id=(x_peer(d), region), device_id_type=MESH,
        )

    def localized(p):
        return pk[p + 1] + LOCAL_WEIGHT * (pk[p] + pk[p + 2])

    def send_share(k, d):
        j = lax.rem(xi + d, XN)
        for i in range(2):
            part[k, d - 1, i] = message(localized(2 * j + i))
        rs_copy(k, d).start()

    def z_copy(k):
        return pltpu.make_async_remote_copy(
            src_ref=z_out.at[k], dst_ref=z_in.at[k], send_sem=z_s.at[k], recv_sem=z_r.at[k],
            device_id=(z_peer, region), device_id_type=MESH,
        )

    def ag_copy(k, d):
        own = pl.ds(2 * xi, 2)
        return pltpu.make_async_remote_copy(
            src_ref=mixbuf.at[k, own], dst_ref=mixbuf.at[k, own],
            send_sem=ag_s.at[k, d - 1], recv_sem=ag_r.at[k, d - 1],
            device_id=(x_peer(d), region), device_id_type=MESH,
        )

    def await_pair(k, g):
        ahead = pick(g, (0, 1, 3, 2))

        @pl.when(g > 0)
        def _():
            d = XN - ahead
            other = pl.ds(2 * lax.rem(xi + ahead, XN), 2)
            pltpu.make_async_remote_copy(
                src_ref=mixbuf.at[k, other], dst_ref=mixbuf.at[k, other],
                send_sem=ag_s.at[k, d - 1], recv_sem=ag_r.at[k, d - 1],
                device_id=(x_peer(1), region), device_id_type=MESH,
            ).wait_recv()

        return lax.rem(xi + ahead, XN)

    def weigh(j):
        for t in range(2):
            lines = pl.ds(pl.multiple_of(j * 256, 256), 256)
            for n in range(2):
                cols = slice(n * 256, (n + 1) * 256)
                applied = jnp.dot(sq[t, lines, :], amat[t, :, cols], preferred_element_type=F32)
                for i in range(2):
                    at = t * 512 + n * 256
                    z = applied[i * 128:(i + 1) * 128]
                    zb[2 * j + i, 0:128, at:at + 256] = z.astype(BF16)

    def quad(p):
        raw = jnp.dot(zb[p, :, 0:512], sr[0, p], preferred_element_type=F32) + jnp.dot(
            zb[p, :, 512:1024], sr[1, p], preferred_element_type=F32
        )
        pk[p + 1] = packed(raw)

    for k in range(OUTER):
        if k == 0:
            for j in range(4):
                weigh(j)
        else:
            @pl.loop(0, 4)
            def _(g):
                j = await_pair(k - 1, g)
                for i in range(2):
                    p = 2 * j + i
                    moved = jnp.dot(mixbuf[k - 1, p], dev[p], preferred_element_type=F32)
                    for t in range(2):
                        for column in range(4):
                            at = t * 512 + column * 128
                            rows = slice(column * 128, (column + 1) * 128)
                            rounded = (cen[p, :, at:at + 128] + moved[:, at:at + 128]).astype(BF16)
                            block = rounded.astype(F32)
                            sq[t, pl.ds(pl.multiple_of(p * 128, 128), 128), rows] = jnp.tanh(
                                block
                            ).astype(BF16)
                            block = block.T
                            x1[t, p, rows, :] = block.astype(BF16)
                            sr[t, p, rows, :] = jnp.tanh(block).astype(BF16)
                weigh(j)

        for p in (0, 7):
            quad(p)
        for side in range(2):
            halo_out[k, side] = message(pk[1 + 7 * side])
        if k == 0:
            pl.semaphore_wait(barrier, XN + 2)
        for side in range(2):
            halo_copy(k, side).start()
        for p in range(1, 7):
            quad(p)

        for d in (2, 1, 3):
            send_share(k, d)

        if k == 0:
            @pl.loop(0, 8)
            def _(p):
                for t in range(2):
                    for column in range(4):
                        block = xin[t, p, column * 128:(column + 1) * 128, :].astype(F32).T
                        centre = jnp.sum(block, axis=0, keepdims=True) * (1.0 / 128)
                        at = t * 512 + column * 128
                        cen[p, :, at:at + 128] = centre
                        dev[p, :, at:at + 128] = (block - centre).astype(BF16)

        sums = [localized(2 * xi + i) for i in range(2)]
        for d in (1, 3, 2):
            rs_copy(k, d).wait_recv()
            for i in range(2):
                sums[i] = sums[i] + rs_in[k, d - 1, i].astype(F32)
        for i in range(2):
            pk[10 + i] = sums[i]
        for edge, i in ((0, 0), (XN - 1, 1)):
            @pl.when(xi == edge)
            def _():
                total = pk[10 + i]
                for j in range(XN):
                    halo_arrival(k, j).wait_recv()
                    total = total + LOCAL_WEIGHT * halo_in[k, j].astype(F32)
                pk[10 + i] = total
        for i in range(2):
            z_out[k, i] = message(pk[10 + i])
        z_copy(k).start()
        z_copy(k).wait_recv()
        mixes = transforms([pk[10 + i] + z_in[k, i].astype(F32) for i in range(2)])
        for i in range(2):
            mixbuf[k, 2 * xi + i] = mixes[i]
        for d in (2, 1, 3):
            ag_copy(k, d).start()

    @pl.loop(0, 4)
    def _(g):
        j = await_pair(OUTER - 1, g)
        for i in range(2):
            p = 2 * j + i
            mix = mixbuf[OUTER - 1, p].astype(F32)
            full = mix + (1.0 - jnp.sum(mix, axis=1, keepdims=True)) * (1.0 / 128)
            both = jnp.concatenate(halves(full), axis=1)
            for t in range(2):
                x = x1[t, p]
                twice = jnp.concatenate([x, x], axis=1)
                moved = lax.dot_general(twice, both, NT, preferred_element_type=F32)
                out[t, p] = moved.astype(BF16)

    for k in range(OUTER):
        for side in range(2):
            halo_copy(k, side).wait_send()
        for d in range(1, XN):
            rs_copy(k, d).wait_send()
            ag_copy(k, d).wait_send()
        z_copy(k).wait_send()


def shards(regions, ensemble, observations, operator_weight, obs_precision, channel_mask):
    slots, patches, rows, members = ensemble.shape
    hbm = pl.BlockSpec(memory_space=pltpu.HBM)
    near = pl.BlockSpec(memory_space=pltpu.VMEM)
    dma, vmem = pltpu.SemaphoreType.DMA, pltpu.VMEM
    return pl.pallas_call(
        functools.partial(kernel, regions),
        out_shape=jax.ShapeDtypeStruct(ensemble.shape, BF16),
        in_specs=[hbm] * 5,
        out_specs=near,
        scratch_shapes=[
            vmem((2, 8, 512, 128), BF16),
            vmem((2, 8, 1024), F32),
            vmem((1024, 512), BF16),
            vmem((8, 128), F32),
            vmem((2, 1024), jnp.int32),
            vmem((2, 1024), F32),
            vmem((2, 512, 1024), BF16),
            vmem((2, 512, 512), BF16),
            vmem((2, 8, 512, 128), BF16),
            vmem((2, 1024, 512), BF16),
            vmem((8, 128, 1024), BF16),
            vmem((8, 1, 1024), F32),
            vmem((8, 144, 1024), BF16),
            vmem((12, 80, 128), F32),
            vmem((2, 8, 512, 128), BF16),
            vmem((2, 2, 80, 128), BF16),
            vmem((2, XN, 80, 128), BF16),
            vmem((2, XN - 1, 2, 80, 128), BF16),
            vmem((2, XN - 1, 2, 80, 128), BF16),
            vmem((2, 2, 80, 128), BF16),
            vmem((2, 2, 80, 128), BF16),
            vmem((2, 8, 128, 128), BF16),
            dma((5,)),
            dma((2, 2)), dma((2, XN)),
            dma((2, XN - 1)), dma((2, XN - 1)),
            dma((2,)), dma((2,)),
            dma((2, XN - 1)), dma((2, XN - 1)),
        ],
        compiler_params=pltpu.CompilerParams(
            collective_id=0, has_side_effects=True, vmem_limit_bytes=40 << 20
        ),
        name="smoother",
    )(
        *(
            pltpu.with_memory_space_constraint(array, pltpu.HBM)
            for array in (
                ensemble, observations, operator_weight, obs_precision.reshape(8, 128), channel_mask
            )
        )
    )


def solution(mesh):
    return jax.shard_map(
        functools.partial(shards, mesh.shape["region"]),
        mesh=mesh,
        in_specs=(
            P("slot", "region", None, None),
            P("slot", "region", None),
            P(),
            P(),
            P("slot", None),
        ),
        out_specs=P("slot", "region", None, None),
        check_vma=False,
    )
```

```python
import functools
import math

import jax
import jax.numpy as jnp
from jax import lax
from jax.experimental import pallas as pl
from jax.experimental.pallas import tpu as pltpu
from jax.sharding import PartitionSpec as P

OUTER = 2
NS_STEPS = 8
LOCAL_WEIGHT = 0.5
XN = 4

F32 = jnp.float32
BF16 = jnp.bfloat16
MESH = pl.DeviceIdType.MESH
NT = (((1,), (1,)), ((), ()))


def iota(shape, dim):
    return lax.broadcasted_iota(jnp.int32, shape, dim)


def halves(a):
    high = a.astype(BF16)
    return high, (a - high.astype(F32)).astype(BF16)


def product(a, b):
    (ah, al), (bh, bl) = a, b
    left = jnp.concatenate([ah, al], axis=1)
    right = jnp.concatenate(
        [jnp.concatenate([bh, bl], axis=1), jnp.concatenate([bh, jnp.zeros_like(bl)], axis=1)],
        axis=0,
    )
    both = jnp.dot(left, right, preferred_element_type=F32)
    return both[:, 0:128] + both[:, 128:256]


def first_term(a, b):
    return jnp.dot(a[0], b[0], preferred_element_type=F32)


def packed(raw):
    first = jnp.sum(raw[0:128], axis=0, keepdims=True) * (1.0 / 128)
    pull = jnp.broadcast_to(raw[128:129] + raw[129:130], (8, 128))
    gram = jnp.concatenate([raw[0:128], pull], axis=0) - first
    gram = gram - jnp.sum(gram, axis=1, keepdims=True) * (1.0 / 128)
    top, bottom = gram[0:64], gram[64:128]
    row, col = iota((64, 128), 0), iota((64, 128), 1)
    body = jnp.where(col >= row, top, pltpu.roll(bottom, 64, 1))
    diag = jnp.sum(jnp.where(col == row + 64, bottom, 0.0), axis=0, keepdims=True)
    tail_row = iota((16, 128), 0)
    grad = gram[128:129]
    tail = jnp.where(tail_row == 0, diag, jnp.where(tail_row == 1, grad, 0.0))
    return jnp.concatenate([body, tail], axis=0)


def message(pack):
    tail = pack[64:80]
    row = iota((16, 128), 0)
    grad = tail[1:2] + tail[2:3]
    high = grad.astype(BF16).astype(F32)
    tail = jnp.where(
        row == 0, tail, jnp.where(row == 1, high, jnp.where(row == 2, grad - high, 0.0))
    )
    return jnp.concatenate([pack[0:64].astype(BF16), tail.astype(BF16)], axis=0)


def unpacked(pack):
    top = pack[0:64]
    row, col = iota((64, 128), 0), iota((64, 128), 1)
    upper = jnp.where(col >= row, top, 0.0)
    lower = pltpu.roll(jnp.where(col < row, top, 0.0), 64, 1)
    lower = jnp.where(col == row + 64, pack[64:65], lower)
    half = jnp.concatenate([upper, lower], axis=0)
    row, col = iota((128, 128), 0), iota((128, 128), 1)
    return jnp.where(row == col, half, half + half.T), pack[65:66] + pack[66:67]


def transforms(packs):
    members = 128
    row, col = iota((128, 128), 0), iota((128, 128), 1)
    identity = jnp.where(row == col, 1.0, 0.0).astype(F32)
    grads, scales, iterates, factors = [], [], [], []
    for pack in packs:
        gram, grad = unpacked(pack)
        shifted = gram + (members - 1.0) * identity
        total = jnp.sum(jnp.sum(shifted * shifted, axis=0, keepdims=True), axis=1, keepdims=True)
        norm = jnp.sqrt(total)
        grads.append(grad)
        scales.append(1.0 / jnp.sqrt(norm))
        iterates.append(shifted * (1.0 / norm))
    count = len(packs)
    middles = [1.5 * identity - 0.5 * it for it in iterates]
    split_mid = [halves(m) for m in middles]
    factors = middles
    iterates = [
        product(
            halves(jnp.concatenate([iterates[i], jnp.broadcast_to(grads[i], (16, 128))], axis=0)),
            split_mid[i],
        )
        for i in range(count)
    ]
    for number in range(1, NS_STEPS):
        split_fac = [halves(f) for f in factors]
        split_it = [halves(it) for it in iterates]
        multiply = first_term if number < NS_STEPS - 2 else product
        middles = [
            1.5 * identity
            - 0.5 * multiply(split_fac[i], tuple(part[0:128] for part in split_it[i]))
            for i in range(count)
        ]
        split_mid = [halves(m) for m in middles]
        if number + 1 == NS_STEPS:
            split_it = [tuple(part[128:144] for part in split) for split in split_it]
        iterates = [product(split_it[i], split_mid[i]) for i in range(count)]
        factors = [product(split_mid[i], split_fac[i]) for i in range(count)]
    out = []
    for i in range(count):
        along = product(halves(iterates[i]), halves(factors[i]))[0:1] * (scales[i] * scales[i])
        out.append((math.sqrt(members - 1.0) * scales[i] * factors[i] + along).astype(BF16))
    return out


def pick(g, values):
    chosen = values[-1]
    for number in range(len(values) - 1):
        chosen = jnp.where(g == number, values[number], chosen)
    return chosen


def kernel(
    regions,
    x_hbm, obs_hbm, op_hbm, prec_hbm, mask_hbm,
    out,
    xin, obs, op, prec, mask, wt, opw, amat,
    sr, sq, dev, cen, zb, pk, x1,
    halo_out, halo_in, part, rs_in, z_out, z_in, mixbuf,
    load_sem, op_sem, halo_s, halo_r, rs_s, rs_r, z_s, z_r, ag_s, ag_r,
):
    slot, region = lax.axis_index("slot"), lax.axis_index("region")
    xi, zi = lax.rem(slot, XN), lax.div(slot, XN)
    z_peer = lax.rem(slot + XN, 2 * XN)
    before, after = lax.rem(region + regions - 1, regions), lax.rem(region + 1, regions)

    def at_x(j):
        return zi * XN + j

    def x_peer(d):
        return at_x(lax.rem(xi + d, XN))

    barrier = pltpu.get_barrier_semaphore()

    def greet(device):
        pl.semaphore_signal(barrier, inc=1, device_id=device, device_id_type=MESH)

    for d in range(1, XN):
        greet((x_peer(d), region))
    greet((z_peer, region))
    for edge, neighbour in ((0, before), (XN - 1, after)):
        @pl.when(xi == edge)
        def _():
            for j in range(XN):
                greet((at_x(j), neighbour))

    def op_load(ci):
        lines = pl.ds(pl.multiple_of(ci * 128, 128), 128)
        return pltpu.make_async_copy(op_hbm.at[lines], op.at[lines], op_sem.at[ci])

    loads = [
        pltpu.make_async_copy(prec_hbm, prec, load_sem.at[0]),
        pltpu.make_async_copy(mask_hbm, mask, load_sem.at[1]),
        pltpu.make_async_copy(obs_hbm, obs, load_sem.at[2]),
        pltpu.make_async_copy(x_hbm, xin, load_sem.at[3]),
    ]
    for load in loads[:2]:
        load.start()
    for ci in range(8):
        op_load(ci).start()
    for load in loads[2:]:
        load.start()
    pk[0] = jnp.zeros((80, 128), F32)
    pk[9] = jnp.zeros((80, 128), F32)
    for load in loads[:2]:
        load.wait()
    for ci in range(8):
        cols = slice(ci * 128, (ci + 1) * 128)
        wt[:, cols] = prec[ci:ci + 1, :] * mask[:, cols].astype(F32) * (1.0 / OUTER)

    @pl.loop(0, 8)
    def _(ci):
        op_load(ci).wait()
        c = pl.multiple_of(ci * 128, 128)
        weight = [wt[t:t + 1, pl.ds(c, 128)] for t in range(2)]
        for ri in range(4):
            block = op[pl.ds(c, 128), ri * 128:(ri + 1) * 128].astype(F32).T
            for t in range(2):
                opw[t, ri * 128:(ri + 1) * 128, pl.ds(c, 128)] = (block * weight[t]).astype(BF16)

    loads[2].wait()
    for t in range(2):
        high, low = halves(obs[t] * wt[t:t + 1, :])
        both = jnp.dot(jnp.concatenate([high, low], axis=0), op[...], preferred_element_type=F32)
        row = iota((16, 512), 0)
        for p in range(8):
            pull = both[p:p + 1] + both[p + 8:p + 9]
            high = pull.astype(BF16).astype(F32)
            tail = jnp.where(row == 0, high, jnp.where(row == 1, pull - high, 0.0))
            zb[p, 128:144, t * 512:(t + 1) * 512] = tail.astype(BF16)

    loads[3].wait()

    @pl.loop(0, 4)
    def _(step):
        t, first = lax.div(step, 2), pl.multiple_of(lax.rem(step, 2) * 256, 256)
        for i in range(2):
            cols = slice(i * 256, (i + 1) * 256)
            amat[t, pl.ds(first, 256), cols] = jnp.dot(
                opw[t, pl.ds(first, 256), :], op[:, cols], preferred_element_type=F32
            ).astype(BF16)
            p = 2 * step + i
            for s in range(2):
                for column in range(4):
                    rows = slice(column * 128, (column + 1) * 128)
                    squashed = jnp.tanh(xin[s, p, rows, :].astype(F32))
                    sr[s, p, rows, :] = squashed.astype(BF16)
                    sq[s, pl.ds(pl.multiple_of(p * 128, 128), 128), rows] = squashed.T.astype(BF16)

    def halo_copy(k, side):
        return pltpu.make_async_remote_copy(
            src_ref=halo_out.at[k, side], dst_ref=halo_in.at[k, xi],
            send_sem=halo_s.at[k, side], recv_sem=halo_r.at[k, xi],
            device_id=(at_x(XN - 1), before) if side == 0 else (at_x(0), after),
            device_id_type=MESH,
        )

    def halo_arrival(k, j):
        return pltpu.make_async_remote_copy(
            src_ref=halo_out.at[k, 0], dst_ref=halo_in.at[k, j],
            send_sem=halo_s.at[k, 0], recv_sem=halo_r.at[k, j],
            device_id=(at_x(0), after), device_id_type=MESH,
        )

    def rs_copy(k, d):
        return pltpu.make_async_remote_copy(
            src_ref=part.at[k, d - 1], dst_ref=rs_in.at[k, d - 1],
            send_sem=rs_s.at[k, d - 1], recv_sem=rs_r.at[k, d - 1],
            device_id=(x_peer(d), region), device_id_type=MESH,
        )

    def localized(p):
        return pk[p + 1] + LOCAL_WEIGHT * (pk[p] + pk[p + 2])

    def send_share(k, d):
        j = lax.rem(xi + d, XN)
        for i in range(2):
            part[k, d - 1, i] = message(localized(2 * j + i))
        rs_copy(k, d).start()

    def z_copy(k):
        return pltpu.make_async_remote_copy(
            src_ref=z_out.at[k], dst_ref=z_in.at[k], send_sem=z_s.at[k], recv_sem=z_r.at[k],
            device_id=(z_peer, region), device_id_type=MESH,
        )

    def ag_copy(k, d):
        own = pl.ds(2 * xi, 2)
        return pltpu.make_async_remote_copy(
            src_ref=mixbuf.at[k, own], dst_ref=mixbuf.at[k, own],
            send_sem=ag_s.at[k, d - 1], recv_sem=ag_r.at[k, d - 1],
            device_id=(x_peer(d), region), device_id_type=MESH,
        )

    def await_pair(k, g):
        ahead = pick(g, (0, 1, 3, 2))

        @pl.when(g > 0)
        def _():
            d = XN - ahead
            other = pl.ds(2 * lax.rem(xi + ahead, XN), 2)
            pltpu.make_async_remote_copy(
                src_ref=mixbuf.at[k, other], dst_ref=mixbuf.at[k, other],
                send_sem=ag_s.at[k, d - 1], recv_sem=ag_r.at[k, d - 1],
                device_id=(x_peer(1), region), device_id_type=MESH,
            ).wait_recv()

        return lax.rem(xi + ahead, XN)

    def weigh(j):
        for t in range(2):
            lines = pl.ds(pl.multiple_of(j * 256, 256), 256)
            for n in range(2):
                cols = slice(n * 256, (n + 1) * 256)
                applied = jnp.dot(sq[t, lines, :], amat[t, :, cols], preferred_element_type=F32)
                for i in range(2):
                    at = t * 512 + n * 256
                    z = applied[i * 128:(i + 1) * 128]
                    zb[2 * j + i, 0:128, at:at + 256] = z.astype(BF16)

    def quad(p):
        raw = jnp.dot(zb[p, :, 0:512], sr[0, p], preferred_element_type=F32) + jnp.dot(
            zb[p, :, 512:1024], sr[1, p], preferred_element_type=F32
        )
        pk[p + 1] = packed(raw)

    def send_edge(k, side):
        quad(7 * side)
        halo_out[k, side] = message(pk[1 + 7 * side])
        halo_copy(k, side).start()

    for k in range(OUTER):
        if k == 0:
            weigh(0)
            weigh(3)
            pl.semaphore_wait(barrier, XN + 2)
            for side in range(2):
                send_edge(k, side)
            weigh(1)
            weigh(2)
        else:
            @pl.loop(0, 4)
            def _(g):
                j = await_pair(k - 1, g)
                for i in range(2):
                    p = 2 * j + i
                    moved = jnp.dot(mixbuf[k - 1, p], dev[p], preferred_element_type=F32)
                    for t in range(2):
                        for column in range(4):
                            at = t * 512 + column * 128
                            rows = slice(column * 128, (column + 1) * 128)
                            rounded = (cen[p, :, at:at + 128] + moved[:, at:at + 128]).astype(BF16)
                            block = rounded.astype(F32)
                            sq[t, pl.ds(pl.multiple_of(p * 128, 128), 128), rows] = jnp.tanh(
                                block
                            ).astype(BF16)
                            block = block.T
                            x1[t, p, rows, :] = block.astype(BF16)
                            sr[t, p, rows, :] = jnp.tanh(block).astype(BF16)
                weigh(j)
                for side in range(2):
                    @pl.when(j == side * (XN - 1))
                    def _():
                        send_edge(k, side)

        for p in range(1, 7):
            quad(p)

        for d in (2, 1, 3):
            send_share(k, d)

        if k == 0:
            @pl.loop(0, 8)
            def _(p):
                for t in range(2):
                    for column in range(4):
                        block = xin[t, p, column * 128:(column + 1) * 128, :].astype(F32).T
                        centre = jnp.sum(block, axis=0, keepdims=True) * (1.0 / 128)
                        at = t * 512 + column * 128
                        cen[p, :, at:at + 128] = centre
                        dev[p, :, at:at + 128] = (block - centre).astype(BF16)

        sums = [localized(2 * xi + i) for i in range(2)]
        for d in (1, 3, 2):
            rs_copy(k, d).wait_recv()
            for i in range(2):
                sums[i] = sums[i] + rs_in[k, d - 1, i].astype(F32)
        for i in range(2):
            pk[10 + i] = sums[i]
        for edge, i in ((0, 0), (XN - 1, 1)):
            @pl.when(xi == edge)
            def _():
                total = pk[10 + i]
                for j in range(XN):
                    halo_arrival(k, j).wait_recv()
                    total = total + LOCAL_WEIGHT * halo_in[k, j].astype(F32)
                pk[10 + i] = total
        for i in range(2):
            z_out[k, i] = message(pk[10 + i])
        z_copy(k).start()
        z_copy(k).wait_recv()
        mixes = transforms([pk[10 + i] + z_in[k, i].astype(F32) for i in range(2)])
        for i in range(2):
            mixbuf[k, 2 * xi + i] = mixes[i]
        for d in (2, 1, 3):
            ag_copy(k, d).start()

    @pl.loop(0, 4)
    def _(g):
        j = await_pair(OUTER - 1, g)
        for i in range(2):
            p = 2 * j + i
            mix = mixbuf[OUTER - 1, p].astype(F32)
            full = mix + (1.0 - jnp.sum(mix, axis=1, keepdims=True)) * (1.0 / 128)
            both = jnp.concatenate(halves(full), axis=1)
            for t in range(2):
                x = x1[t, p]
                twice = jnp.concatenate([x, x], axis=1)
                moved = lax.dot_general(twice, both, NT, preferred_element_type=F32)
                out[t, p] = moved.astype(BF16)

    for k in range(OUTER):
        for side in range(2):
            halo_copy(k, side).wait_send()
        for d in range(1, XN):
            rs_copy(k, d).wait_send()
            ag_copy(k, d).wait_send()
        z_copy(k).wait_send()


def shards(regions, ensemble, observations, operator_weight, obs_precision, channel_mask):
    slots, patches, rows, members = ensemble.shape
    hbm = pl.BlockSpec(memory_space=pltpu.HBM)
    near = pl.BlockSpec(memory_space=pltpu.VMEM)
    dma, vmem = pltpu.SemaphoreType.DMA, pltpu.VMEM
    return pl.pallas_call(
        functools.partial(kernel, regions),
        out_shape=jax.ShapeDtypeStruct(ensemble.shape, BF16),
        in_specs=[hbm] * 5,
        out_specs=near,
        scratch_shapes=[
            vmem((2, 8, 512, 128), BF16),
            vmem((2, 8, 1024), F32),
            vmem((1024, 512), BF16),
            vmem((8, 128), F32),
            vmem((2, 1024), jnp.int32),
            vmem((2, 1024), F32),
            vmem((2, 512, 1024), BF16),
            vmem((2, 512, 512), BF16),
            vmem((2, 8, 512, 128), BF16),
            vmem((2, 1024, 512), BF16),
            vmem((8, 128, 1024), BF16),
            vmem((8, 1, 1024), F32),
            vmem((8, 144, 1024), BF16),
            vmem((12, 80, 128), F32),
            vmem((2, 8, 512, 128), BF16),
            vmem((2, 2, 80, 128), BF16),
            vmem((2, XN, 80, 128), BF16),
            vmem((2, XN - 1, 2, 80, 128), BF16),
            vmem((2, XN - 1, 2, 80, 128), BF16),
            vmem((2, 2, 80, 128), BF16),
            vmem((2, 2, 80, 128), BF16),
            vmem((2, 8, 128, 128), BF16),
            dma((4,)), dma((8,)),
            dma((2, 2)), dma((2, XN)),
            dma((2, XN - 1)), dma((2, XN - 1)),
            dma((2,)), dma((2,)),
            dma((2, XN - 1)), dma((2, XN - 1)),
        ],
        compiler_params=pltpu.CompilerParams(
            collective_id=0, has_side_effects=True, vmem_limit_bytes=40 << 20
        ),
        name="smoother",
    )(
        *(
            pltpu.with_memory_space_constraint(array, pltpu.HBM)
            for array in (
                ensemble, observations, operator_weight, obs_precision.reshape(8, 128), channel_mask
            )
        )
    )


def solution(mesh):
    return jax.shard_map(
        functools.partial(shards, mesh.shape["region"]),
        mesh=mesh,
        in_specs=(
            P("slot", "region", None, None),
            P("slot", "region", None),
            P(),
            P(),
            P("slot", None),
        ),
        out_specs=P("slot", "region", None, None),
        check_vma=False,
    )
```

```python
import functools
import math

import jax
import jax.numpy as jnp
from jax import lax
from jax.experimental import pallas as pl
from jax.experimental.pallas import tpu as pltpu
from jax.sharding import PartitionSpec as P

OUTER = 2
NS_STEPS = 8
LOCAL_WEIGHT = 0.5
XN = 4

F32 = jnp.float32
BF16 = jnp.bfloat16
MESH = pl.DeviceIdType.MESH
NT = (((1,), (1,)), ((), ()))


def iota(shape, dim):
    return lax.broadcasted_iota(jnp.int32, shape, dim)


def halves(a):
    high = a.astype(BF16)
    return high, (a - high.astype(F32)).astype(BF16)


def product(a, b):
    (ah, al), (bh, bl) = a, b
    left = jnp.concatenate([ah, al], axis=1)
    right = jnp.concatenate(
        [jnp.concatenate([bh, bl], axis=1), jnp.concatenate([bh, jnp.zeros_like(bl)], axis=1)],
        axis=0,
    )
    both = jnp.dot(left, right, preferred_element_type=F32)
    return both[:, 0:128] + both[:, 128:256]


def first_term(a, b):
    return jnp.dot(a[0], b[0], preferred_element_type=F32)


def packed(raw):
    first = jnp.sum(raw[0:128], axis=0, keepdims=True) * (1.0 / 128)
    pull = jnp.broadcast_to(raw[128:129] + raw[129:130], (8, 128))
    gram = jnp.concatenate([raw[0:128], pull], axis=0) - first
    gram = gram - jnp.sum(gram, axis=1, keepdims=True) * (1.0 / 128)
    top, bottom = gram[0:64], gram[64:128]
    row, col = iota((64, 128), 0), iota((64, 128), 1)
    body = jnp.where(col >= row, top, pltpu.roll(bottom, 64, 1))
    diag = jnp.sum(jnp.where(col == row + 64, bottom, 0.0), axis=0, keepdims=True)
    tail_row = iota((16, 128), 0)
    grad = gram[128:129]
    tail = jnp.where(tail_row == 0, diag, jnp.where(tail_row == 1, grad, 0.0))
    return jnp.concatenate([body, tail], axis=0)


def message(pack):
    tail = pack[64:80]
    row = iota((16, 128), 0)
    grad = tail[1:2] + tail[2:3]
    high = grad.astype(BF16).astype(F32)
    tail = jnp.where(
        row == 0, tail, jnp.where(row == 1, high, jnp.where(row == 2, grad - high, 0.0))
    )
    return jnp.concatenate([pack[0:64].astype(BF16), tail.astype(BF16)], axis=0)


def unpacked(pack):
    top = pack[0:64]
    row, col = iota((64, 128), 0), iota((64, 128), 1)
    upper = jnp.where(col >= row, top, 0.0)
    lower = pltpu.roll(jnp.where(col < row, top, 0.0), 64, 1)
    lower = jnp.where(col == row + 64, pack[64:65], lower)
    half = jnp.concatenate([upper, lower], axis=0)
    row, col = iota((128, 128), 0), iota((128, 128), 1)
    return jnp.where(row == col, half, half + half.T), pack[65:66] + pack[66:67]


def transforms(packs):
    members = 128
    row, col = iota((128, 128), 0), iota((128, 128), 1)
    identity = jnp.where(row == col, 1.0, 0.0).astype(F32)
    grads, scales, iterates, factors = [], [], [], []
    for pack in packs:
        gram, grad = unpacked(pack)
        shifted = gram + (members - 1.0) * identity
        total = jnp.sum(jnp.sum(shifted * shifted, axis=0, keepdims=True), axis=1, keepdims=True)
        norm = jnp.sqrt(total)
        grads.append(grad)
        scales.append(1.0 / jnp.sqrt(norm))
        iterates.append(shifted * (1.0 / norm))
    count = len(packs)
    middles = [1.5 * identity - 0.5 * it for it in iterates]
    split_mid = [halves(m) for m in middles]
    factors = middles
    iterates = [
        product(
            halves(jnp.concatenate([iterates[i], jnp.broadcast_to(grads[i], (16, 128))], axis=0)),
            split_mid[i],
        )
        for i in range(count)
    ]
    for number in range(1, NS_STEPS):
        split_fac = [halves(f) for f in factors]
        split_it = [halves(it) for it in iterates]
        multiply = first_term if number < NS_STEPS - 2 else product
        middles = [
            1.5 * identity
            - 0.5 * multiply(split_fac[i], tuple(part[0:128] for part in split_it[i]))
            for i in range(count)
        ]
        split_mid = [halves(m) for m in middles]
        if number + 1 == NS_STEPS:
            split_it = [tuple(part[128:144] for part in split) for split in split_it]
        iterates = [product(split_it[i], split_mid[i]) for i in range(count)]
        factors = [product(split_mid[i], split_fac[i]) for i in range(count)]
    out = []
    for i in range(count):
        along = product(halves(iterates[i]), halves(factors[i]))[0:1] * (scales[i] * scales[i])
        out.append((math.sqrt(members - 1.0) * scales[i] * factors[i] + along).astype(BF16))
    return out


def pick(g, values):
    chosen = values[-1]
    for number in range(len(values) - 1):
        chosen = jnp.where(g == number, values[number], chosen)
    return chosen


def kernel(
    regions,
    x_hbm, obs_hbm, op_hbm, prec_hbm, mask_hbm,
    out,
    xin, obs, op, prec, mask, wt, opw, amat,
    sr, sq, dev, cen, zb, pk, x1,
    halo_out, halo_in, part, rs_in, z_out, z_in, mixbuf,
    load_sem, op_sem, halo_s, halo_r, rs_s, rs_r, z_s, z_r, ag_s, ag_r,
):
    slot, region = lax.axis_index("slot"), lax.axis_index("region")
    xi, zi = lax.rem(slot, XN), lax.div(slot, XN)
    z_peer = lax.rem(slot + XN, 2 * XN)
    before, after = lax.rem(region + regions - 1, regions), lax.rem(region + 1, regions)

    def at_x(j):
        return zi * XN + j

    def x_peer(d):
        return at_x(lax.rem(xi + d, XN))

    barrier = pltpu.get_barrier_semaphore()

    def greet(device):
        pl.semaphore_signal(barrier, inc=1, device_id=device, device_id_type=MESH)

    for d in range(1, XN):
        greet((x_peer(d), region))
    greet((z_peer, region))
    for edge, neighbour in ((0, before), (XN - 1, after)):
        @pl.when(xi == edge)
        def _():
            for j in range(XN):
                greet((at_x(j), neighbour))

    def op_load(ci):
        lines = pl.ds(pl.multiple_of(ci * 128, 128), 128)
        return pltpu.make_async_copy(op_hbm.at[lines], op.at[lines], op_sem.at[ci])

    loads = [
        pltpu.make_async_copy(prec_hbm, prec, load_sem.at[0]),
        pltpu.make_async_copy(mask_hbm, mask, load_sem.at[1]),
        pltpu.make_async_copy(obs_hbm, obs, load_sem.at[2]),
        pltpu.make_async_copy(x_hbm, xin, load_sem.at[3]),
    ]
    for load in loads[:2]:
        load.start()
    for ci in range(8):
        op_load(ci).start()
    for load in loads[2:]:
        load.start()
    pk[0] = jnp.zeros((80, 128), F32)
    pk[9] = jnp.zeros((80, 128), F32)
    for load in loads[:2]:
        load.wait()
    for ci in range(8):
        cols = slice(ci * 128, (ci + 1) * 128)
        wt[:, cols] = prec[ci:ci + 1, :] * mask[:, cols].astype(F32) * (1.0 / OUTER)

    @pl.loop(0, 8)
    def _(ci):
        op_load(ci).wait()
        c = pl.multiple_of(ci * 128, 128)
        weight = [wt[t:t + 1, pl.ds(c, 128)] for t in range(2)]
        for ri in range(4):
            block = op[pl.ds(c, 128), ri * 128:(ri + 1) * 128].astype(F32).T
            for t in range(2):
                opw[t, ri * 128:(ri + 1) * 128, pl.ds(c, 128)] = (block * weight[t]).astype(BF16)

    loads[2].wait()
    for t in range(2):
        high, low = halves(obs[t] * wt[t:t + 1, :])
        both = jnp.dot(jnp.concatenate([high, low], axis=0), op[...], preferred_element_type=F32)
        row = iota((16, 512), 0)
        for p in range(8):
            pull = both[p:p + 1] + both[p + 8:p + 9]
            high = pull.astype(BF16).astype(F32)
            tail = jnp.where(row == 0, high, jnp.where(row == 1, pull - high, 0.0))
            zb[p, 128:144, t * 512:(t + 1) * 512] = tail.astype(BF16)

    loads[3].wait()

    @pl.loop(0, 4)
    def _(step):
        t, first = lax.div(step, 2), pl.multiple_of(lax.rem(step, 2) * 256, 256)
        for i in range(2):
            cols = slice(i * 256, (i + 1) * 256)
            amat[t, pl.ds(first, 256), cols] = jnp.dot(
                opw[t, pl.ds(first, 256), :], op[:, cols], preferred_element_type=F32
            ).astype(BF16)
            p = 2 * step + i
            for s in range(2):
                for column in range(4):
                    rows = slice(column * 128, (column + 1) * 128)
                    squashed = jnp.tanh(xin[s, p, rows, :].astype(F32))
                    sr[s, p, rows, :] = squashed.astype(BF16)
                    sq[s, pl.ds(pl.multiple_of(p * 128, 128), 128), rows] = squashed.T.astype(BF16)

    def halo_copy(k, side):
        return pltpu.make_async_remote_copy(
            src_ref=halo_out.at[k, side], dst_ref=halo_in.at[k, xi],
            send_sem=halo_s.at[k, side], recv_sem=halo_r.at[k, xi],
            device_id=(at_x(XN - 1), before) if side == 0 else (at_x(0), after),
            device_id_type=MESH,
        )

    def halo_arrival(k, j):
        return pltpu.make_async_remote_copy(
            src_ref=halo_out.at[k, 0], dst_ref=halo_in.at[k, j],
            send_sem=halo_s.at[k, 0], recv_sem=halo_r.at[k, j],
            device_id=(at_x(0), after), device_id_type=MESH,
        )

    def rs_copy(k, d):
        return pltpu.make_async_remote_copy(
            src_ref=part.at[k, d - 1], dst_ref=rs_in.at[k, d - 1],
            send_sem=rs_s.at[k, d - 1], recv_sem=rs_r.at[k, d - 1],
            device_id=(x_peer(d), region), device_id_type=MESH,
        )

    def localized(p):
        return pk[p + 1] + LOCAL_WEIGHT * (pk[p] + pk[p + 2])

    def send_share(k, d):
        j = lax.rem(xi + d, XN)
        for i in range(2):
            part[k, d - 1, i] = message(localized(2 * j + i))
        rs_copy(k, d).start()

    def z_copy(k):
        return pltpu.make_async_remote_copy(
            src_ref=z_out.at[k], dst_ref=z_in.at[k], send_sem=z_s.at[k], recv_sem=z_r.at[k],
            device_id=(z_peer, region), device_id_type=MESH,
        )

    def ag_copy(k, d):
        own = pl.ds(2 * xi, 2)
        return pltpu.make_async_remote_copy(
            src_ref=mixbuf.at[k, own], dst_ref=mixbuf.at[k, own],
            send_sem=ag_s.at[k, d - 1], recv_sem=ag_r.at[k, d - 1],
            device_id=(x_peer(d), region), device_id_type=MESH,
        )

    def await_pair(k, g):
        ahead = pick(g, (0, 1, 3, 2))

        @pl.when(g > 0)
        def _():
            d = XN - ahead
            other = pl.ds(2 * lax.rem(xi + ahead, XN), 2)
            pltpu.make_async_remote_copy(
                src_ref=mixbuf.at[k, other], dst_ref=mixbuf.at[k, other],
                send_sem=ag_s.at[k, d - 1], recv_sem=ag_r.at[k, d - 1],
                device_id=(x_peer(1), region), device_id_type=MESH,
            ).wait_recv()

        return lax.rem(xi + ahead, XN)

    def weigh(j):
        for t in range(2):
            lines = pl.ds(pl.multiple_of(j * 256, 256), 256)
            for n in range(2):
                cols = slice(n * 256, (n + 1) * 256)
                applied = jnp.dot(sq[t, lines, :], amat[t, :, cols], preferred_element_type=F32)
                for i in range(2):
                    at = t * 512 + n * 256
                    z = applied[i * 128:(i + 1) * 128]
                    zb[2 * j + i, 0:128, at:at + 256] = z.astype(BF16)

    def quad(p):
        raw = jnp.dot(zb[p, :, 0:512], sr[0, p], preferred_element_type=F32) + jnp.dot(
            zb[p, :, 512:1024], sr[1, p], preferred_element_type=F32
        )
        pk[p + 1] = packed(raw)

    def send_edge(k, side):
        quad(7 * side)
        halo_out[k, side] = message(pk[1 + 7 * side])
        halo_copy(k, side).start()

    for k in range(OUTER):
        if k == 0:
            weigh(0)
            weigh(3)
            pl.semaphore_wait(barrier, XN + 2)
            for side in range(2):
                send_edge(k, side)
            weigh(1)
            weigh(2)
        else:
            @pl.loop(0, 4)
            def _(g):
                j = await_pair(k - 1, g)
                for i in range(2):
                    p = 2 * j + i
                    moved = jnp.dot(mixbuf[k - 1, p], dev[p], preferred_element_type=F32)
                    for t in range(2):
                        for column in range(4):
                            at = t * 512 + column * 128
                            rows = slice(column * 128, (column + 1) * 128)
                            rounded = (cen[p, :, at:at + 128] + moved[:, at:at + 128]).astype(BF16)
                            block = rounded.astype(F32)
                            sq[t, pl.ds(pl.multiple_of(p * 128, 128), 128), rows] = jnp.tanh(
                                block
                            ).astype(BF16)
                            block = block.T
                            x1[t, p, rows, :] = block.astype(BF16)
                            sr[t, p, rows, :] = jnp.tanh(block).astype(BF16)
                weigh(j)

            for side in range(2):
                send_edge(k, side)

        for p in range(1, 7):
            quad(p)

        for d in (2, 1, 3):
            send_share(k, d)

        if k == 0:
            @pl.loop(0, 8)
            def _(p):
                for t in range(2):
                    for column in range(4):
                        block = xin[t, p, column * 128:(column + 1) * 128, :].astype(F32).T
                        centre = jnp.sum(block, axis=0, keepdims=True) * (1.0 / 128)
                        at = t * 512 + column * 128
                        cen[p, :, at:at + 128] = centre
                        dev[p, :, at:at + 128] = (block - centre).astype(BF16)

        sums = [localized(2 * xi + i) for i in range(2)]
        for d in (1, 3, 2):
            rs_copy(k, d).wait_recv()
            for i in range(2):
                sums[i] = sums[i] + rs_in[k, d - 1, i].astype(F32)
        for i in range(2):
            pk[10 + i] = sums[i]
        for edge, i in ((0, 0), (XN - 1, 1)):
            @pl.when(xi == edge)
            def _():
                total = pk[10 + i]
                for j in range(XN):
                    halo_arrival(k, j).wait_recv()
                    total = total + LOCAL_WEIGHT * halo_in[k, j].astype(F32)
                pk[10 + i] = total
        for i in range(2):
            z_out[k, i] = message(pk[10 + i])
        z_copy(k).start()
        z_copy(k).wait_recv()
        mixes = transforms([pk[10 + i] + z_in[k, i].astype(F32) for i in range(2)])
        for i in range(2):
            mixbuf[k, 2 * xi + i] = mixes[i]
        for d in (2, 1, 3):
            ag_copy(k, d).start()

    @pl.loop(0, 4)
    def _(g):
        j = await_pair(OUTER - 1, g)
        for i in range(2):
            p = 2 * j + i
            mix = mixbuf[OUTER - 1, p].astype(F32)
            full = mix + (1.0 - jnp.sum(mix, axis=1, keepdims=True)) * (1.0 / 128)
            both = jnp.concatenate(halves(full), axis=1)
            for t in range(2):
                x = x1[t, p]
                twice = jnp.concatenate([x, x], axis=1)
                moved = lax.dot_general(twice, both, NT, preferred_element_type=F32)
                out[t, p] = moved.astype(BF16)

    for k in range(OUTER):
        for side in range(2):
            halo_copy(k, side).wait_send()
        for d in range(1, XN):
            rs_copy(k, d).wait_send()
            ag_copy(k, d).wait_send()
        z_copy(k).wait_send()


def shards(regions, ensemble, observations, operator_weight, obs_precision, channel_mask):
    slots, patches, rows, members = ensemble.shape
    hbm = pl.BlockSpec(memory_space=pltpu.HBM)
    near = pl.BlockSpec(memory_space=pltpu.VMEM)
    dma, vmem = pltpu.SemaphoreType.DMA, pltpu.VMEM
    return pl.pallas_call(
        functools.partial(kernel, regions),
        out_shape=jax.ShapeDtypeStruct(ensemble.shape, BF16),
        in_specs=[hbm] * 5,
        out_specs=near,
        scratch_shapes=[
            vmem((2, 8, 512, 128), BF16),
            vmem((2, 8, 1024), F32),
            vmem((1024, 512), BF16),
            vmem((8, 128), F32),
            vmem((2, 1024), jnp.int32),
            vmem((2, 1024), F32),
            vmem((2, 512, 1024), BF16),
            vmem((2, 512, 512), BF16),
            vmem((2, 8, 512, 128), BF16),
            vmem((2, 1024, 512), BF16),
            vmem((8, 128, 1024), BF16),
            vmem((8, 1, 1024), F32),
            vmem((8, 144, 1024), BF16),
            vmem((12, 80, 128), F32),
            vmem((2, 8, 512, 128), BF16),
            vmem((2, 2, 80, 128), BF16),
            vmem((2, XN, 80, 128), BF16),
            vmem((2, XN - 1, 2, 80, 128), BF16),
            vmem((2, XN - 1, 2, 80, 128), BF16),
            vmem((2, 2, 80, 128), BF16),
            vmem((2, 2, 80, 128), BF16),
            vmem((2, 8, 128, 128), BF16),
            dma((4,)), dma((8,)),
            dma((2, 2)), dma((2, XN)),
            dma((2, XN - 1)), dma((2, XN - 1)),
            dma((2,)), dma((2,)),
            dma((2, XN - 1)), dma((2, XN - 1)),
        ],
        compiler_params=pltpu.CompilerParams(
            collective_id=0, has_side_effects=True, vmem_limit_bytes=40 << 20
        ),
        name="smoother",
    )(
        *(
            pltpu.with_memory_space_constraint(array, pltpu.HBM)
            for array in (
                ensemble, observations, operator_weight, obs_precision.reshape(8, 128), channel_mask
            )
        )
    )


def solution(mesh):
    return jax.shard_map(
        functools.partial(shards, mesh.shape["region"]),
        mesh=mesh,
        in_specs=(
            P("slot", "region", None, None),
            P("slot", "region", None),
            P(),
            P(),
            P("slot", None),
        ),
        out_specs=P("slot", "region", None, None),
        check_vma=False,
    )
```
